32 devices in a mesh: gx: 2 (over x), gy: 4 (over z), wa: 4 (over y, core).
Axes of the slice: x: 2, y: 2, z: 4, core: 2. Of those that a mesh axis runs over, the one named last changes fastest.
Arguments:
- velocity: float32 [3, 64, 256, 512], P(None, 'gx', 'gy', 'wa'), may hold values from -70 to 70, as said below
- lengths: int32 [2, 4, 4, 2048], P('gx', 'gy', 'wa'), may hold values from 16 to 128
- destinations: int32 [2, 4, 4, 2048, 1], P('gx', 'gy', 'wa'), may hold values from 0 to 7; in each aligned block of 2048 rows (0 to 2047, 2048 to 4095, ..., all dimensions but the last counted through in order) at most 512 rows name the same one
Outputs:
- received: float32 [8, 4, 3, 8, 512, 128], P(('gx', 'gy'), 'wa')
The draws below stay inside these ranges and needn't reach their ends.
Inputs may be any that keep to these rules, and one draw needn't show every extreme that they name: `velocity`: finite values; the amplitude varies over the grid. `destinations`: in every draw no device sends more than 512 blocks to one writer, and some device sends exactly 512 to one writer.
All inputs are finite; a program needn't handle non-finite values.
Results may differ from the reference program's by a relative error of at most 0.0003.
Values sent between devices are 32-bit elements; how exact they have to be, the bound alone decides.
A program may use at most 128 MiB of HBM per device.

```python
import math
import jax
import jax.numpy as jnp
import numpy as np
from jax import lax

CX = 32
CY = 64
CZ = 128
COMP = 3
BY = 8
BZ = 16
COEF = 128
NBLK = 2048
WRITERS = 8
CAP = 512
NX = 64
NY = 256
NZ = 512
N_GX = 2
N_GY = 4
N_WA = 4


def draw_velocity(key, part):
    xs = jnp.arange(NX, dtype=jnp.float32)[:, None, None] / NX
    ys = jnp.arange(NY, dtype=jnp.float32)[None, :, None] / NY
    noise = jax.random.truncated_normal(key, -6.0, 6.0, (COMP, NX, NY, NZ), jnp.float32)
    amplitude = jnp.exp(jnp.log(10.0) * 0.5 * (xs + ys))
    return amplitude * noise


def place_ends(entries, rng, least, high):
    shape = entries.shape
    spot = [jax.random.randint(jax.random.fold_in(rng, axis), (), 0, shape[axis]) for axis in range(len(shape))]
    entries = entries.at[tuple(spot)].set(least)
    longest = shape.index(max(shape))
    spot[longest] = (spot[longest] + 1) % shape[longest]
    return entries.at[tuple(spot)].set(high)


def shared_out(own_key, own, number, rows, number_of, top, bound, skew):
    sequence = jax.random.permutation(own_key, number_of)
    crowded, usual = load_shares(number_of, rows * top, bound, skew, True), load_shares(number_of, rows * top, bound, skew, False)
    places = jnp.arange(number_of)

    def named(tallies, turn):
        used = int((tallies > 0).sum())
        fixed = max(1, used // 4)
        passed = fixed + (places - fixed + turn * (used - fixed)) % max(1, number_of - fixed)
        return jnp.zeros((number_of,), jnp.int32).at[sequence[jnp.where(places < fixed, places, passed)]].set(jnp.asarray(tallies, jnp.int32))

    tallies = jnp.where(number % 4 == 0, named(crowded, number // 4), named(usual, number - number // 4 - 1))
    mixed = jax.random.permutation(jax.random.fold_in(own, 3), number_of)
    giver, receiver = mixed[0:number_of // 2 * 2:2], mixed[1:number_of // 2 * 2:2]
    room = jnp.minimum(tallies[giver] - 1, bound - tallies[receiver]) // 2
    room = jnp.where((giver == sequence[0]) | (receiver == sequence[0]) | (tallies[receiver] == 0), 0, jnp.maximum(room, 0))
    passed = jax.random.randint(jax.random.fold_in(own, 4), (number_of // 2,), 0, 1 << 20) % (room + 1)
    tallies = tallies.at[giver].add(-passed).at[receiver].add(passed)
    members = jnp.searchsorted(jnp.cumsum(tallies), jnp.arange(rows * top), side="right").astype(jnp.int32)
    grid = members.reshape(top, rows).T
    grid = grid[jax.random.permutation(jax.random.fold_in(own, 1), rows)]
    turn = jax.random.randint(jax.random.fold_in(own, 2), (rows, 1), 0, top)
    return jnp.take_along_axis(grid, (jnp.arange(top)[None, :] + turn) % top, axis=1)


def load_shares(count, total, reach, lean, full):
    weights = [(1 << 20) // math.isqrt(standing ** lean) + 1 for standing in range(1, count + 1)]
    largest = reach if full else min(reach, max(-(-total // count), total * weights[0] // sum(weights)))
    least = 1 if total - largest >= count - 1 else 0
    given, spare = [largest] + [least] * (count - 1), total - largest - least * (count - 1)
    while spare > 0:
        free = [i for i in range(1, count) if given[i] < largest] or [i for i in range(1, count) if given[i] < reach]
        pool, budget = sum([weights[i] for i in free]), spare
        for i in free:
            more = min(reach - given[i], max(1, budget * weights[i] // pool), spare)
            given[i] = given[i] + more
            spare = spare - more
    return np.array(given)


def setup_inputs(seed: int = 0) -> dict:
    key_list = jax.random.split(jax.random.key(seed), 4)
    velocity = draw_velocity(jax.random.fold_in(key_list[3], 71), 0)
    lengths = place_ends(jax.random.randint(key_list[1], (N_GX, N_GY, N_WA, NBLK), 16, COEF + 1), jax.random.fold_in(key_list[1], 1), 16, COEF).astype(jnp.int32)
    destinations_keys = jax.random.split(jax.random.fold_in(key_list[2], 1), N_GX * N_GY * N_WA * NBLK // NBLK)
    destinations_turns = jax.random.permutation(jax.random.fold_in(key_list[2], 3), N_GX * N_GY * N_WA * NBLK // NBLK)
    destinations = jax.vmap(lambda own, number: shared_out(jax.random.fold_in(key_list[2], 2), own, number, NBLK, WRITERS, 1, CAP, 2))(destinations_keys, destinations_turns).reshape((N_GX, N_GY, N_WA, NBLK, 1))
    return dict(velocity=velocity, lengths=lengths, destinations=destinations)


def dct_table(count):
    freqs = jnp.arange(count, dtype=jnp.float32)[:, None]
    points = jnp.arange(count, dtype=jnp.float32)[None, :]
    table = jnp.cos(jnp.pi * (points + 0.5) * freqs / count) * jnp.sqrt(2.0 / count)
    return jnp.where(freqs == 0.0, table * jnp.sqrt(0.5), table)

def curl_field(padded):

    def along_x(component):
        return (padded[component, 2:, 1:-1, 1:-1] - padded[component, :-2, 1:-1, 1:-1]) * 0.5

    def along_y(component):
        return (padded[component, 1:-1, 2:, 1:-1] - padded[component, 1:-1, :-2, 1:-1]) * 0.5

    def along_z(component):
        return (padded[component, 1:-1, 1:-1, 2:] - padded[component, 1:-1, 1:-1, :-2]) * 0.5
    first = along_y(2) - along_z(1)
    second = along_z(0) - along_x(2)
    third = along_x(1) - along_y(0)
    return jnp.stack([first, second, third])

def place_blocks(scaled, lens, targets):
    onehot = (targets[:, None] == jnp.arange(WRITERS, dtype=jnp.int32)[None, :]).astype(jnp.int32)
    before = jnp.cumsum(onehot, axis=0) - onehot
    ranking = lax.optimization_barrier(jnp.sum(before * onehot, axis=1))
    slot_index = (targets * CAP + ranking).astype(jnp.int32)
    buffer = jnp.zeros((WRITERS * CAP, COMP, COEF), jnp.float32)
    buffer = buffer.at[slot_index].set(scaled)
    return buffer.reshape(WRITERS, CAP, COMP, COEF)

def reference(velocity, lengths, destinations):
    padded = jnp.pad(velocity, ((0, 0), (1, 1), (1, 1), (1, 1)), mode='wrap')
    curl = curl_field(padded)
    total = jnp.sum(curl * curl)
    rms = jnp.sqrt(total / (COMP * NX * NY * NZ) + 1e-06)
    kron_table = jnp.kron(dct_table(BY), dct_table(BZ))
    grouped = curl.reshape(COMP, N_GX, CX, N_GY, CY // BY, BY, N_WA, CZ // BZ, BZ)
    grouped = grouped.transpose(1, 3, 6, 2, 4, 7, 0, 5, 8)
    blocks = grouped.reshape(-1, COEF)
    coeffs = jnp.dot(blocks, kron_table.T, precision=lax.Precision.HIGHEST, preferred_element_type=jnp.float32)
    coeffs = coeffs.reshape(N_GX * N_GY * N_WA, NBLK, COMP, COEF)
    freqs = jnp.arange(COEF, dtype=jnp.int32)
    lens = lengths.reshape(N_GX * N_GY * N_WA, NBLK)
    keep = (freqs[None, None, None, :] < lens[:, :, None, None]).astype(jnp.float32)
    scaled = coeffs * keep / rms
    targets = destinations.reshape(N_GX * N_GY * N_WA, NBLK)
    buffers = jax.vmap(place_blocks)(scaled, lens, targets)
    buffers = buffers.reshape(WRITERS, N_WA, WRITERS, CAP, COMP, COEF)
    return buffers.transpose(2, 1, 4, 0, 3, 5)
```

```python
import functools

import jax
import jax.numpy as jnp
import numpy as np
from jax import lax
from jax.experimental import pallas as pl
from jax.experimental.pallas import tpu as pltpu
from jax.sharding import PartitionSpec as P

BY = 8
BZ = 16
UNROLL = 2
MESH = pl.DeviceIdType.MESH


def dct_table(count):
    freqs, points = np.arange(count)[:, None], np.arange(count)[None, :]
    table = np.cos(np.pi * (points + 0.5) * freqs / count) * np.sqrt(2.0 / count)
    return np.where(freqs == 0, table * np.sqrt(0.5), table)


def split_table():
    kron = np.kron(dct_table(BY), dct_table(BZ)).T.astype(np.float32)
    high = kron.astype(jnp.bfloat16)
    low = (kron - high.astype(np.float32)).astype(jnp.bfloat16)
    return np.block([[high, low], [high, np.zeros_like(low)]]).astype(jnp.bfloat16)


def faces_kernel(
    writers, capacity, pitch, targets, lens, vel, words, spots, blank, y_faces, z_faces, need
):
    comps, cells_x, cells_y, cells_z = vel.shape
    lane = lax.broadcasted_iota(jnp.int32, (cells_y, cells_z), 1)

    def plane(x, acc):
        here = lane == x
        rolled = [
            pltpu.roll(vel[comp, x], lax.rem(x + last, cells_z), 1)
            for last in range(2)
            for comp in (0, 1)
        ]
        for i, comp in enumerate((0, 2)):
            y_faces[0, i, pl.ds(x, 1), :] = vel[comp, x, 0:1]
            y_faces[1, i, pl.ds(x, 1), :] = vel[comp, x, cells_y - 1 : cells_y]
        return tuple(jnp.where(here, new, old) for new, old in zip(rolled, acc))

    zero = jnp.zeros((cells_y, cells_z), jnp.float32)
    columns = lax.fori_loop(0, cells_x, plane, (zero,) * 4, unroll=4)
    for last in range(2):
        for i in range(2):
            z_faces[last, i] = columns[2 * last + i]

    t, kept = targets[...], lens[...]
    rows, lanes = t.shape
    shape = (lanes, lanes)
    upper = (
        lax.broadcasted_iota(jnp.int32, shape, 0) < lax.broadcasted_iota(jnp.int32, shape, 1)
    ).astype(jnp.float32).astype(jnp.bfloat16)
    square = (rows, rows)
    lower = (
        lax.broadcasted_iota(jnp.int32, square, 1) < lax.broadcasted_iota(jnp.int32, square, 0)
    ).astype(jnp.float32).astype(jnp.bfloat16)
    weight = kept.astype(jnp.float32)

    def body(w, acc):
        spot, start, most = acc
        mine = t == w
        ones = mine.astype(jnp.float32)
        sizes = jnp.where(mine, weight, 0.0)
        both = jnp.concatenate([ones, sizes], axis=0).astype(jnp.bfloat16)
        inner = jnp.dot(both, upper, preferred_element_type=jnp.float32)
        side = jnp.concatenate([ones, sizes], axis=1).astype(jnp.bfloat16)
        before = jnp.dot(lower, side, preferred_element_type=jnp.float32)
        rank = inner[:rows] + jnp.sum(before[:, :lanes], axis=1, keepdims=True)
        offset = inner[rows:] + jnp.sum(before[:, lanes:], axis=1, keepdims=True)
        spot = jnp.where(mine, w * capacity + rank.astype(jnp.int32), spot)
        start = jnp.where(mine, w * pitch + offset.astype(jnp.int32), start)
        most = jnp.where(mine, offset + weight, most)
        return spot, start, most

    none = jnp.zeros_like(t)
    spot, start, most = lax.fori_loop(
        0, writers, body, (none, none, jnp.zeros(t.shape, jnp.float32)), unroll=8
    )
    spots[...] = spot
    words[...] = start * 256 + kept
    need[...] = jnp.max(most.reshape(rows // 8, 8, lanes), axis=0)
    place = lax.broadcasted_iota(jnp.int32, blank.shape, 0) * lanes + lax.broadcasted_iota(
        jnp.int32, blank.shape, 1
    )
    blank[...] = lax.div(place, capacity) * (pitch * 256)


def plane_peers(n_x, n_y):
    a, b, c = (lax.axis_index(axis) for axis in ("gx", "gy", "wa"))
    offsets = [(i, j) for i in range(n_x) for j in range(n_y) if i or j]
    offsets.sort(key=lambda o: (bool(o[0]) and bool(o[1]), min(o[1], n_y - o[1])))
    return [(lax.rem(a + i, n_x), lax.rem(b + j, n_y), c) for i, j in offsets]


def line_mates(n_z):
    a, b, c = (lax.axis_index(axis) for axis in ("gx", "gy", "wa"))
    return [(a, b, lax.rem(c + k, n_z)) for k in range(1, n_z)]


def send_to(src, dst, send_sem, recv_sem, device):
    copy = pltpu.make_async_remote_copy(
        src_ref=src,
        dst_ref=dst,
        send_sem=send_sem,
        recv_sem=recv_sem,
        device_id=device,
        device_id_type=MESH,
    )
    copy.start()
    return copy


def halo_kernel(
    sizes, tiers, vel, y_faces, z_faces, need, halos, tier, near, far, send_sem, recv_sem, part_send,
    part_recv, own_sem,
):
    place = [lax.axis_index(axis) for axis in ("gx", "gy", "wa")]
    n_x, n_y, n_z = sizes
    cells_x = vel.shape[1]

    def beside(axis, step):
        size = sizes[axis]
        moved = lax.rem(place[axis] + step + size, size)
        return tuple(moved if i == axis else p for i, p in enumerate(place))

    across, along = pl.ds(0, vel.shape[2]), pl.ds(0, cells_x)
    moves = [
        (vel.at[pl.ds(1, 2), cells_x - 1], halos.at[0, :, across], beside(0, 1)),
        (vel.at[pl.ds(1, 2), 0], halos.at[1, :, across], beside(0, -1)),
        (y_faces.at[1], halos.at[2, :, along], beside(1, 1)),
        (y_faces.at[0], halos.at[3, :, along], beside(1, -1)),
        (z_faces.at[1], halos.at[4, :, across], beside(2, 1)),
        (z_faces.at[0], halos.at[5, :, across], beside(2, -1)),
    ]
    peers, mates = plane_peers(n_x, n_y), line_mates(n_z)
    others = [device for _, _, device in moves] + peers + mates
    barrier = pltpu.get_barrier_semaphore()
    for device in others:
        pl.semaphore_signal(barrier, inc=1, device_id=device, device_id_type=MESH)
    pl.semaphore_wait(barrier, len(others))
    c = place[2]
    own = pltpu.make_async_copy(need, near.at[c], own_sem)
    own.start()
    first = [
        send_to(need, near.at[c], part_send.at[k], part_recv.at[k], device)
        for k, device in enumerate(mates)
    ]
    copies = [
        send_to(src, dst, send_sem.at[k], recv_sem.at[k], device)
        for k, (src, dst, device) in enumerate(moves)
    ]
    own.wait()
    for copy in first:
        copy.wait()
    for k, device in enumerate(peers):
        sem = n_z - 1 + k
        copies.append(send_to(near, far.at[k], part_send.at[sem], part_recv.at[sem], device))
    for copy in copies:
        copy.wait()
    most = jnp.maximum(jnp.max(near[...], axis=0), jnp.max(far[...], axis=(0, 1)))
    above = jnp.max(most)
    tier[0] = sum((above > 128.0 * rows).astype(jnp.int32) for rows in tiers[:-1])


def block_rows(plane):
    cells_y, cells_z = plane.shape
    tiles = plane.reshape(cells_y // BY, BY, cells_z)
    sub = lax.broadcasted_iota(jnp.int32, tiles.shape, 1)
    group = lax.broadcasted_iota(jnp.int32, tiles.shape, 2) // BZ
    k = 1
    while k < BY:
        s_bit, g_bit = (sub & k) != 0, (group & k) != 0
        fwd = pltpu.roll(pltpu.roll(tiles, BY - k, 1), k * BZ, 2)
        back = pltpu.roll(pltpu.roll(tiles, k, 1), cells_z - k * BZ, 2)
        tiles = jnp.where(s_bit == g_bit, tiles, jnp.where(g_bit, fwd, back))
        k *= 2
    return tiles.reshape(cells_y, cells_z)


def blocks_kernel(words, spots, blank, vel, halos, table, out, squares, meta, coeffs, meta_sem):
    comps, cells_x, cells_y, cells_z = vel.shape
    nblk = coeffs.shape[0] // comps
    per_plane = nblk // cells_x
    width = out.shape[1]
    row = lax.broadcasted_iota(jnp.int32, (cells_y, cells_z), 0)
    lane = lax.broadcasted_iota(jnp.int32, (cells_y, cells_z), 1)
    clear = pltpu.make_async_copy(blank, meta, meta_sem)
    clear.start()

    def plane(x, acc):
        u, v, w = vel[0, x], vel[1, x], vel[2, x]

        def along_x(comp):
            nxt = jnp.where(
                x == cells_x - 1, halos[1, comp - 1, :cells_y], vel[comp, jnp.minimum(x + 1, cells_x - 1)]
            )
            prv = jnp.where(x == 0, halos[0, comp - 1, :cells_y], vel[comp, jnp.maximum(x - 1, 0)])
            return (nxt - prv) * 0.5

        def along_y(f, face):
            nxt = jnp.where(
                row == cells_y - 1, halos[3, face, pl.ds(x, 1), :], pltpu.roll(f, cells_y - 1, 0)
            )
            prv = jnp.where(row == 0, halos[2, face, pl.ds(x, 1), :], pltpu.roll(f, 1, 0))
            return (nxt - prv) * 0.5

        def along_z(f, face):
            after = pltpu.roll(halos[5, face, :cells_y], cells_z - 1 - x, 1)
            before = pltpu.roll(halos[4, face, :cells_y], lax.rem(cells_z - x, cells_z), 1)
            nxt = jnp.where(lane == cells_z - 1, after, pltpu.roll(f, cells_z - 1, 1))
            prv = jnp.where(lane == 0, before, pltpu.roll(f, 1, 1))
            return (nxt - prv) * 0.5

        curl = (
            along_y(w, 1) - along_z(v, 1),
            along_z(u, 0) - along_x(2),
            along_x(1) - along_y(u, 0),
        )
        for c in curl:
            acc = acc + jnp.sum((c * c).reshape(cells_y // 8, 8, cells_z), axis=0)
        flat = jnp.concatenate([block_rows(c) for c in curl], axis=0)
        high = flat.astype(jnp.bfloat16)
        low = (flat - high.astype(jnp.float32)).astype(jnp.bfloat16)
        both = jnp.dot(
            jnp.concatenate([high, low], axis=1), table[...], preferred_element_type=jnp.float32
        )
        result = both[:, :width] + both[:, width:]
        start = x * (comps * per_plane)
        for c in range(comps):
            coeffs[pl.ds(start + c, per_plane, stride=comps), :] = result[
                c * per_plane : (c + 1) * per_plane
            ]
        return acc

    spread = lax.broadcasted_iota(jnp.int32, (comps, width), 1)
    group = 8

    def place(x):
        for start in range(0, per_plane, group):
            found = []
            for k in range(start, min(start + group, per_plane)):
                i = x * per_plane + k
                word = words[i]
                meta[spots[i]] = word
                shift = lax.shift_right_logical(word, 8) & (width - 1)
                row = lax.shift_right_logical(word, 15) * comps
                moved = pltpu.roll(coeffs[pl.ds(i * comps, comps), :], shift, 1)
                found.append((row, moved, spread >= shift))
            for row, moved, mask in found:
                pltpu.store(out.at[pl.ds(row, comps), :], moved, mask=mask)
                out[pl.ds(row + comps, comps), :] = moved

    together = next(n for n in (UNROLL, 2, 1) if cells_x % n == 0)

    def step(t, acc):
        for k in range(together):
            place((t - 1) * together + k)
        return planes(t, acc)

    def planes(t, acc):
        for k in range(together):
            acc = plane(t * together + k, acc)
        return acc

    clear.wait()
    first = planes(0, jnp.zeros((8, cells_z), jnp.float32))
    squares[...] = lax.fori_loop(1, cells_x // together, step, first)
    for k in range(together):
        place(cells_x - together + k)


def exchange_kernel(
    n_x, n_y, n_z, rows, send, squares, meta, recv, total, heard, near, far, send_sem, recv_sem,
    part_send, part_recv, word_send, word_recv, own_sem,
):
    a, b = lax.axis_index("gx"), lax.axis_index("gy")
    c = lax.axis_index("wa")
    me = a * n_y + b
    peers, mates = plane_peers(n_x, n_y), line_mates(n_z)
    barrier = pltpu.get_barrier_semaphore()
    for device in mates + peers:
        pl.semaphore_signal(barrier, inc=1, device_id=device, device_id_type=MESH)
    pl.semaphore_wait(barrier, len(peers) + len(mates))
    used = pl.ds(0, rows)

    own = [
        pltpu.make_async_copy(squares, near.at[c], own_sem.at[0]),
        pltpu.make_async_copy(meta.at[me], heard.at[me], own_sem.at[1]),
        pltpu.make_async_copy(send.at[me, used], recv.at[me, used], own_sem.at[2]),
    ]
    for copy in own:
        copy.start()
    first = [
        send_to(squares, near.at[c], part_send.at[k], part_recv.at[k], device)
        for k, device in enumerate(mates)
    ]

    def number(device):
        return device[0] * n_y + device[1]

    def blocks_to(k):
        device = peers[k]
        return send_to(
            send.at[number(device), used], recv.at[me, used], send_sem.at[k], recv_sem.at[k], device
        )

    copies = [
        send_to(meta.at[number(device)], heard.at[me], word_send.at[k], word_recv.at[k], device)
        for k, device in enumerate(peers)
    ]
    ahead = min(3, len(peers))
    copies += [blocks_to(k) for k in range(ahead)]
    own[0].wait()
    for copy in first:
        copy.wait()
    for k, device in enumerate(peers):
        sem = n_z - 1 + k
        copies.append(send_to(near, far.at[k], part_send.at[sem], part_recv.at[sem], device))
    copies += [blocks_to(k) for k in range(ahead, len(peers))]
    for copy in own[1:]:
        copy.wait()
    for copy in copies:
        copy.wait()
    total[...] = jnp.sum(near[...], axis=0) + jnp.sum(far[...], axis=(0, 1))


def unpack_kernel(every, n_y, pitch, meta, squares, recv, out, scale):
    comps, _, capacity, width = out.shape
    source = pl.program_id(0)
    base = (lax.axis_index("gx") * n_y + lax.axis_index("gy")) * pitch

    @pl.when(source == 0)
    def _():
        total = jnp.sum(squares[...], keepdims=True)
        scale[...] = jnp.broadcast_to(1.0 / jnp.sqrt(total / every + 1e-06), scale.shape)

    lane = lax.broadcasted_iota(jnp.int32, (comps, width), 1)
    factor = scale[:comps]
    group = 16 if capacity % 16 == 0 else 8

    def some(t, _):
        found = []
        for k in range(group):
            slot = t * group + k
            word = meta[source * capacity + slot]
            length = word & 255
            shift = lax.shift_right_logical(word, 8) & (width - 1)
            row = (lax.shift_right_logical(word, 15) - base) * comps
            head = recv[0, pl.ds(row, comps), :]
            tail = recv[0, pl.ds(row + comps, comps), :]
            joined = jnp.where(lane >= shift, head, tail)
            moved = pltpu.roll(joined, (width - shift) & (width - 1), 1)
            found.append((slot, jnp.where(lane < length, moved * factor, 0.0)))
        for slot, value in found:
            for c in range(comps):
                out[c, 0, pl.ds(slot, 1), :] = value[c : c + 1]
        return 0

    lax.fori_loop(0, capacity // group, some, 0)


def tier_rows(capacity):
    steps = (16, 18, 19, 20, 22, 24, 28, 32)
    return sorted({-(-capacity * step // (32 * 8)) * 8 for step in steps})


def local(velocity, lengths, destinations):
    n_x, n_y, n_z = lax.axis_size("gx"), lax.axis_size("gy"), lax.axis_size("wa")
    comps, cells_x, cells_y, cells_z = velocity.shape
    width = BY * BZ
    nblk = cells_x * cells_y * cells_z // width
    writers = n_x * n_y
    capacity = max(2, 2 * nblk // writers)
    region = capacity + 8
    f32 = jnp.float32
    tiers = tier_rows(capacity)

    smem = pl.BlockSpec(memory_space=pltpu.SMEM)
    vmem = pl.BlockSpec(memory_space=pltpu.VMEM)
    anywhere = pl.BlockSpec(memory_space=pl.ANY)
    dma = pltpu.SemaphoreType.DMA
    flat = jax.ShapeDtypeStruct((nblk // 128, 128), jnp.int32)
    words, spots, blank, y_faces, z_faces, need = pl.pallas_call(
        functools.partial(faces_kernel, writers, capacity, region * width),
        out_shape=(
            flat,
            flat,
            jax.ShapeDtypeStruct((writers * capacity // 128, 128), jnp.int32),
            jax.ShapeDtypeStruct((2, 2, cells_x, cells_z), f32),
            jax.ShapeDtypeStruct((2, 2, cells_y, cells_z), f32),
            jax.ShapeDtypeStruct((8, 128), f32),
        ),
        name="faces",
    )(destinations.reshape(nblk // 128, 128), lengths.reshape(nblk // 128, 128), velocity)
    halos, tier = pl.pallas_call(
        functools.partial(halo_kernel, (n_x, n_y, n_z), tiers),
        out_shape=(
            jax.ShapeDtypeStruct((6, 2, max(cells_x, cells_y), cells_z), f32),
            jax.ShapeDtypeStruct((1,), jnp.int32),
        ),
        in_specs=[anywhere] * 3 + [vmem],
        out_specs=(anywhere, smem),
        scratch_shapes=[
            pltpu.VMEM((n_z,) + need.shape, f32),
            pltpu.VMEM((writers - 1, n_z) + need.shape, f32),
            dma((6,)),
            dma((6,)),
            dma((writers + n_z - 2,)),
            dma((writers + n_z - 2,)),
            dma,
        ],
        compiler_params=pltpu.CompilerParams(collective_id=1, has_side_effects=True),
        name="halo",
    )(velocity, y_faces, z_faces, need)

    table = jnp.asarray(split_table())
    outgoing, squares, meta = pl.pallas_call(
        blocks_kernel,
        out_shape=(
            jax.ShapeDtypeStruct((writers * region * comps, width), f32),
            jax.ShapeDtypeStruct((8, cells_z), f32),
            jax.ShapeDtypeStruct((writers * capacity,), jnp.int32),
        ),
        in_specs=[smem, smem] + [anywhere] + [vmem] * 3,
        out_specs=(vmem, vmem, smem),
        scratch_shapes=[pltpu.VMEM((nblk * comps, width), f32), dma],
        compiler_params=pltpu.CompilerParams(vmem_limit_bytes=48 * 2**20),
        name="blocks",
    )(
        words.reshape(nblk),
        spots.reshape(nblk),
        blank.reshape(writers * capacity),
        velocity,
        halos,
        table,
    )
    outgoing = outgoing.reshape(writers, region * comps, width)
    part = min(capacity, 128)
    meta = meta.reshape(writers, capacity // part, part)

    def exchange(index, outgoing, squares, meta):
        rows = tiers[index] * comps
        return pl.pallas_call(
            functools.partial(exchange_kernel, n_x, n_y, n_z, rows),
            out_shape=(
                jax.ShapeDtypeStruct(outgoing.shape, f32),
                jax.ShapeDtypeStruct(squares.shape, f32),
                jax.ShapeDtypeStruct(meta.shape, jnp.int32),
            ),
            in_specs=[anywhere, vmem, anywhere],
            out_specs=(anywhere, vmem, anywhere),
            scratch_shapes=[
                pltpu.VMEM((n_z,) + squares.shape, f32),
                pltpu.VMEM((writers - 1, n_z) + squares.shape, f32),
                dma((writers - 1,)),
                dma((writers - 1,)),
                dma((writers + n_z - 2,)),
                dma((writers + n_z - 2,)),
                dma((writers - 1,)),
                dma((writers - 1,)),
                dma((3,)),
            ],
            compiler_params=pltpu.CompilerParams(collective_id=2 + index, has_side_effects=True),
            name=f"exchange{tiers[index]}",
        )(outgoing, squares, meta)

    branches = [functools.partial(exchange, index) for index in range(len(tiers))]
    arrived, squares, heard = lax.switch(tier[0], branches, outgoing, squares, meta)

    every = velocity.size * n_x * n_y * n_z
    received = pl.pallas_call(
        functools.partial(unpack_kernel, float(every), n_y, region),
        grid=(writers,),
        in_specs=[
            smem,
            pl.BlockSpec((8, cells_z), lambda s: (0, 0)),
            pl.BlockSpec((1, region * comps, width), lambda s: (s, 0, 0)),
        ],
        out_specs=pl.BlockSpec((comps, 1, capacity, width), lambda s: (0, s, 0, 0)),
        out_shape=jax.ShapeDtypeStruct((comps, writers, capacity, width), f32),
        scratch_shapes=[pltpu.VMEM((8, width), f32)],
        name="unpack",
    )(heard.reshape(writers * capacity), squares, arrived)
    return received.reshape(1, 1, comps, writers, capacity, width)


def solution(mesh):
    return jax.shard_map(
        local,
        mesh=mesh,
        in_specs=(
            P(None, "gx", "gy", "wa"),
            P("gx", "gy", "wa", None),
            P("gx", "gy", "wa", None, None),
        ),
        out_specs=P(("gx", "gy"), "wa", None, None, None, None),
        check_vma=False,
    )
```

```python
import functools
import math

import jax
import jax.numpy as jnp
import numpy as np
from jax import lax
from jax.experimental import pallas as pl
from jax.experimental.pallas import tpu as pltpu
from jax.sharding import PartitionSpec as P

BY = 8
BZ = 16
UNROLL = 2
MESH = pl.DeviceIdType.MESH


def dct_table(count):
    freqs, points = np.arange(count)[:, None], np.arange(count)[None, :]
    table = np.cos(np.pi * (points + 0.5) * freqs / count) * np.sqrt(2.0 / count)
    return np.where(freqs == 0, table * np.sqrt(0.5), table)


def split_table():
    kron = np.kron(dct_table(BY), dct_table(BZ)).T.astype(np.float32)
    high = kron.astype(jnp.bfloat16)
    low = (kron - high.astype(np.float32)).astype(jnp.bfloat16)
    return np.block([[high, low], [high, np.zeros_like(low)]]).astype(jnp.bfloat16)


def faces_kernel(
    writers, capacity, region, targets, lens, vel, plan, y_faces, z_faces, need
):
    comps, cells_x, cells_y, cells_z = vel.shape
    lane = lax.broadcasted_iota(jnp.int32, (cells_y, cells_z), 1)

    def plane(x, acc):
        here = lane == x
        rolled = [
            pltpu.roll(vel[comp, x], lax.rem(x + last, cells_z), 1)
            for last in range(2)
            for comp in (0, 1)
        ]
        for i, comp in enumerate((0, 2)):
            y_faces[0, i, pl.ds(x, 1), :] = vel[comp, x, 0:1]
            y_faces[1, i, pl.ds(x, 1), :] = vel[comp, x, cells_y - 1 : cells_y]
        return tuple(jnp.where(here, new, old) for new, old in zip(rolled, acc))

    zero = jnp.zeros((cells_y, cells_z), jnp.float32)
    columns = lax.fori_loop(0, cells_x, plane, (zero,) * 4, unroll=4)
    for last in range(2):
        for i in range(2):
            z_faces[last, i] = columns[2 * last + i]

    t, kept = targets[...], lens[...]
    rows, lanes = t.shape
    shape = (lanes, lanes)
    upper = (
        lax.broadcasted_iota(jnp.int32, shape, 0) < lax.broadcasted_iota(jnp.int32, shape, 1)
    ).astype(jnp.float32).astype(jnp.bfloat16)
    square = (rows, rows)
    lower = (
        lax.broadcasted_iota(jnp.int32, square, 1) < lax.broadcasted_iota(jnp.int32, square, 0)
    ).astype(jnp.float32).astype(jnp.bfloat16)
    weight = kept.astype(jnp.float32)

    def body(w, acc):
        spot, start, site = acc
        mine = t == w
        ones = mine.astype(jnp.float32)
        sizes = jnp.where(mine, weight, 0.0)
        both = jnp.concatenate([ones, sizes], axis=0).astype(jnp.bfloat16)
        inner = jnp.dot(both, upper, preferred_element_type=jnp.float32)
        side = jnp.concatenate([ones, sizes], axis=1).astype(jnp.bfloat16)
        before = jnp.dot(lower, side, preferred_element_type=jnp.float32)
        rank = inner[:rows] + jnp.sum(before[:, :lanes], axis=1, keepdims=True)
        offset = inner[rows:] + jnp.sum(before[:, lanes:], axis=1, keepdims=True)
        spot = jnp.where(mine, w * capacity + rank.astype(jnp.int32), spot)
        offset = offset.astype(jnp.int32)
        start = jnp.where(mine, offset, start)
        site = jnp.where(mine, w * region, site)
        return spot, start, site

    none = jnp.zeros_like(t)
    spot, start, site = lax.fori_loop(0, writers, body, (none, none, none), unroll=8)
    shift = start & (lanes - 1)
    row = lax.shift_right_logical(start, lanes.bit_length() - 1)
    plan[2] = spot
    plan[0] = (row + site) * (comps << 16) + shift
    plan[1] = row * (comps << 16) + (lanes - shift) * 256 + kept
    most = (start + kept).astype(jnp.float32)
    need[...] = jnp.max(most.reshape(rows // 8, 8, lanes), axis=0)


def plane_peers(n_x, n_y):
    a, b, c = (lax.axis_index(axis) for axis in ("gx", "gy", "wa"))
    offsets = [(i, j) for i in range(n_x) for j in range(n_y) if i or j]
    offsets.sort(key=lambda o: (bool(o[0]) and bool(o[1]), min(o[1], n_y - o[1])))
    return [(lax.rem(a + i, n_x), lax.rem(b + j, n_y), c) for i, j in offsets]


def line_mates(n_z):
    a, b, c = (lax.axis_index(axis) for axis in ("gx", "gy", "wa"))
    return [(a, b, lax.rem(c + k, n_z)) for k in range(1, n_z)]


def send_to(src, dst, send_sem, recv_sem, device):
    copy = pltpu.make_async_remote_copy(
        src_ref=src,
        dst_ref=dst,
        send_sem=send_sem,
        recv_sem=recv_sem,
        device_id=device,
        device_id_type=MESH,
    )
    copy.start()
    return copy


def halo_kernel(
    sizes, tiers, vel, y_faces, z_faces, need, halos, tier, near, far, send_sem, recv_sem, part_send,
    part_recv, own_sem,
):
    place = [lax.axis_index(axis) for axis in ("gx", "gy", "wa")]
    n_x, n_y, n_z = sizes
    cells_x = vel.shape[1]

    def beside(axis, step):
        size = sizes[axis]
        moved = lax.rem(place[axis] + step + size, size)
        return tuple(moved if i == axis else p for i, p in enumerate(place))

    across, along = pl.ds(0, vel.shape[2]), pl.ds(0, cells_x)
    moves = [
        (vel.at[pl.ds(1, 2), cells_x - 1], halos.at[0, :, across], beside(0, 1)),
        (vel.at[pl.ds(1, 2), 0], halos.at[1, :, across], beside(0, -1)),
        (y_faces.at[1], halos.at[2, :, along], beside(1, 1)),
        (y_faces.at[0], halos.at[3, :, along], beside(1, -1)),
        (z_faces.at[1], halos.at[4, :, across], beside(2, 1)),
        (z_faces.at[0], halos.at[5, :, across], beside(2, -1)),
    ]
    peers, mates = plane_peers(n_x, n_y), line_mates(n_z)
    others = [device for _, _, device in moves] + peers + mates
    barrier = pltpu.get_barrier_semaphore()
    for device in others:
        pl.semaphore_signal(barrier, inc=1, device_id=device, device_id_type=MESH)
    pl.semaphore_wait(barrier, len(others))
    c = place[2]
    own = pltpu.make_async_copy(need, near.at[c], own_sem)
    own.start()
    first = [
        send_to(need, near.at[c], part_send.at[k], part_recv.at[k], device)
        for k, device in enumerate(mates)
    ]
    copies = [
        send_to(src, dst, send_sem.at[k], recv_sem.at[k], device)
        for k, (src, dst, device) in enumerate(moves)
    ]
    own.wait()
    for copy in first:
        copy.wait()
    for k, device in enumerate(peers):
        sem = n_z - 1 + k
        copies.append(send_to(near, far.at[k], part_send.at[sem], part_recv.at[sem], device))
    for copy in copies:
        copy.wait()
    most = jnp.maximum(jnp.max(near[...], axis=0), jnp.max(far[...], axis=(0, 1)))
    above = jnp.max(most)
    tier[0] = sum((above > 128.0 * rows).astype(jnp.int32) for rows in tiers[:-1])


def block_rows(plane):
    cells_y, cells_z = plane.shape
    tiles = plane.reshape(cells_y // BY, BY, cells_z)
    sub = lax.broadcasted_iota(jnp.int32, tiles.shape, 1)
    group = lax.broadcasted_iota(jnp.int32, tiles.shape, 2) // BZ
    k = 1
    while k < BY:
        s_bit, g_bit = (sub & k) != 0, (group & k) != 0
        fwd = pltpu.roll(pltpu.roll(tiles, BY - k, 1), k * BZ, 2)
        back = pltpu.roll(pltpu.roll(tiles, k, 1), cells_z - k * BZ, 2)
        tiles = jnp.where(s_bit == g_bit, tiles, jnp.where(g_bit, fwd, back))
        k *= 2
    return tiles.reshape(cells_y, cells_z)


def blocks_kernel(
    lists, blank, vel, halos, table, out, squares, meta, coeffs, plan, meta_sem, plan_sem
):
    comps, cells_x, cells_y, cells_z = vel.shape
    nblk = coeffs.shape[0] // comps
    per_plane = nblk // cells_x
    width = out.shape[1]
    row = lax.broadcasted_iota(jnp.int32, (cells_y, cells_z), 0)
    lane = lax.broadcasted_iota(jnp.int32, (cells_y, cells_z), 1)
    clear = pltpu.make_async_copy(blank, meta, meta_sem)
    clear.start()
    fetch = pltpu.make_async_copy(lists, plan, plan_sem)
    fetch.start()

    def plane(x, acc):
        u, v, w = vel[0, x], vel[1, x], vel[2, x]

        def along_x(comp):
            nxt = jnp.where(
                x == cells_x - 1, halos[1, comp - 1, :cells_y], vel[comp, jnp.minimum(x + 1, cells_x - 1)]
            )
            prv = jnp.where(x == 0, halos[0, comp - 1, :cells_y], vel[comp, jnp.maximum(x - 1, 0)])
            return (nxt - prv) * 0.5

        def along_y(f, face):
            nxt = jnp.where(
                row == cells_y - 1, halos[3, face, pl.ds(x, 1), :], pltpu.roll(f, cells_y - 1, 0)
            )
            prv = jnp.where(row == 0, halos[2, face, pl.ds(x, 1), :], pltpu.roll(f, 1, 0))
            return (nxt - prv) * 0.5

        def along_z(f, face):
            after = pltpu.roll(halos[5, face, :cells_y], cells_z - 1 - x, 1)
            before = pltpu.roll(halos[4, face, :cells_y], lax.rem(cells_z - x, cells_z), 1)
            nxt = jnp.where(lane == cells_z - 1, after, pltpu.roll(f, cells_z - 1, 1))
            prv = jnp.where(lane == 0, before, pltpu.roll(f, 1, 1))
            return (nxt - prv) * 0.5

        curl = (
            along_y(w, 1) - along_z(v, 1),
            along_z(u, 0) - along_x(2),
            along_x(1) - along_y(u, 0),
        )
        for c in curl:
            acc = acc + jnp.sum((c * c).reshape(cells_y // 8, 8, cells_z), axis=0)
        flat = jnp.concatenate([block_rows(c) for c in curl], axis=0)
        high = flat.astype(jnp.bfloat16)
        low = (flat - high.astype(jnp.float32)).astype(jnp.bfloat16)
        both = jnp.dot(
            jnp.concatenate([high, low], axis=1), table[...], preferred_element_type=jnp.float32
        )
        result = both[:, :width] + both[:, width:]
        start = x * (comps * per_plane)
        for c in range(comps):
            coeffs[pl.ds(start + c, per_plane, stride=comps), :] = result[
                c * per_plane : (c + 1) * per_plane
            ]
        return acc

    spread = lax.broadcasted_iota(jnp.int32, (comps, width), 1)
    group = 8

    def place(x):
        for start in range(0, per_plane, group):
            found = []
            for k in range(start, min(start + group, per_plane)):
                i = x * per_plane + k
                word = plan[i]
                meta[plan[2 * nblk + i]] = plan[nblk + i]
                shift = word & (width - 1)
                row = lax.shift_right_logical(word, 16)
                moved = pltpu.roll(coeffs[pl.ds(i * comps, comps), :], shift, 1)
                found.append((row, moved, spread >= shift))
            for row, moved, mask in found:
                pltpu.store(out.at[pl.ds(row, comps), :], moved, mask=mask)
                out[pl.ds(row + comps, comps), :] = moved

    together = next(n for n in (UNROLL, 2, 1) if cells_x % n == 0)

    def step(t, acc):
        for k in range(together):
            place((t - 1) * together + k)
        return planes(t, acc)

    def planes(t, acc):
        for k in range(together):
            acc = plane(t * together + k, acc)
        return acc

    clear.wait()
    fetch.wait()
    first = planes(0, jnp.zeros((8, cells_z), jnp.float32))
    squares[...] = lax.fori_loop(1, cells_x // together, step, first)
    for k in range(together):
        place(cells_x - together + k)


def exchange_kernel(
    n_x, n_y, n_z, rows, send, squares, meta, recv, total, heard, near, far, send_sem, recv_sem,
    part_send, part_recv, word_send, word_recv, own_sem,
):
    a, b = lax.axis_index("gx"), lax.axis_index("gy")
    c = lax.axis_index("wa")
    me = a * n_y + b
    peers, mates = plane_peers(n_x, n_y), line_mates(n_z)
    barrier = pltpu.get_barrier_semaphore()
    for device in mates + peers:
        pl.semaphore_signal(barrier, inc=1, device_id=device, device_id_type=MESH)
    pl.semaphore_wait(barrier, len(peers) + len(mates))
    used = pl.ds(0, rows)

    own = [
        pltpu.make_async_copy(squares, near.at[c], own_sem.at[0]),
        pltpu.make_async_copy(meta.at[me], heard.at[me], own_sem.at[1]),
        pltpu.make_async_copy(send.at[me, used], recv.at[me, used], own_sem.at[2]),
    ]
    for copy in own:
        copy.start()
    first = [
        send_to(squares, near.at[c], part_send.at[k], part_recv.at[k], device)
        for k, device in enumerate(mates)
    ]

    def number(device):
        return device[0] * n_y + device[1]

    def blocks_to(k):
        device = peers[k]
        return send_to(
            send.at[number(device), used], recv.at[me, used], send_sem.at[k], recv_sem.at[k], device
        )

    copies = [
        send_to(meta.at[number(device)], heard.at[me], word_send.at[k], word_recv.at[k], device)
        for k, device in enumerate(peers)
    ]
    ahead = min(3, len(peers))
    copies += [blocks_to(k) for k in range(ahead)]
    own[0].wait()
    for copy in first:
        copy.wait()
    for k, device in enumerate(peers):
        sem = n_z - 1 + k
        copies.append(send_to(near, far.at[k], part_send.at[sem], part_recv.at[sem], device))
    copies += [blocks_to(k) for k in range(ahead, len(peers))]
    for copy in own[1:]:
        copy.wait()
    for copy in copies:
        copy.wait()
    total[...] = jnp.sum(near[...], axis=0) + jnp.sum(far[...], axis=(0, 1))


def unpack_kernel(every, meta, squares, recv, out, scale):
    comps, _, capacity, width = out.shape
    source = pl.program_id(0)

    @pl.when(source == 0)
    def _():
        total = jnp.sum(squares[...], keepdims=True)
        scale[...] = jnp.broadcast_to(1.0 / jnp.sqrt(total / every + 1e-06), scale.shape)

    lane = lax.broadcasted_iota(jnp.int32, (comps, width), 1)
    factor = scale[:comps]
    group = math.gcd(capacity, 32)
    first = source * capacity

    def some(t, _):
        start = first + t * group
        for k in range(group):
            mark = meta[start + k]
            fields = jnp.full((comps, width), mark, jnp.int32)
            ahead = lane + (lax.shift_right_logical(fields, 8) & 255)
            row = lax.shift_right_logical(mark, 16)
            head = recv[0, pl.ds(row, comps), :]
            tail = recv[0, pl.ds(row + comps, comps), :]
            joined = jnp.where(ahead >= width, head, tail)
            moved = pltpu.roll(joined, lax.shift_right_logical(mark, 8) & (width - 1), 1)
            value = jnp.where(lane < (fields & 255), moved * factor, 0.0)
            for c in range(comps):
                out[c, 0, pl.ds(t * group + k, 1), :] = value[c : c + 1]
        return 0

    lax.fori_loop(0, capacity // group, some, 0)


def tier_rows(capacity):
    steps = (16, 18, 19, 20, 22, 24, 28, 32)
    return sorted({-(-capacity * step // (32 * 8)) * 8 for step in steps})


def local(velocity, lengths, destinations):
    n_x, n_y, n_z = lax.axis_size("gx"), lax.axis_size("gy"), lax.axis_size("wa")
    comps, cells_x, cells_y, cells_z = velocity.shape
    width = BY * BZ
    nblk = cells_x * cells_y * cells_z // width
    writers = n_x * n_y
    capacity = max(2, 2 * nblk // writers)
    region = capacity + 8
    f32 = jnp.float32
    tiers = tier_rows(capacity)

    smem = pl.BlockSpec(memory_space=pltpu.SMEM)
    vmem = pl.BlockSpec(memory_space=pltpu.VMEM)
    anywhere = pl.BlockSpec(memory_space=pl.ANY)
    dma = pltpu.SemaphoreType.DMA
    plan, y_faces, z_faces, need = pl.pallas_call(
        functools.partial(faces_kernel, writers, capacity, region),
        out_shape=(
            jax.ShapeDtypeStruct((3, nblk // 128, 128), jnp.int32),
            jax.ShapeDtypeStruct((2, 2, cells_x, cells_z), f32),
            jax.ShapeDtypeStruct((2, 2, cells_y, cells_z), f32),
            jax.ShapeDtypeStruct((8, 128), f32),
        ),
        name="faces",
    )(destinations.reshape(nblk // 128, 128), lengths.reshape(nblk // 128, 128), velocity)
    halos, tier = pl.pallas_call(
        functools.partial(halo_kernel, (n_x, n_y, n_z), tiers),
        out_shape=(
            jax.ShapeDtypeStruct((6, 2, max(cells_x, cells_y), cells_z), f32),
            jax.ShapeDtypeStruct((1,), jnp.int32),
        ),
        in_specs=[anywhere] * 3 + [vmem],
        out_specs=(anywhere, smem),
        scratch_shapes=[
            pltpu.VMEM((n_z,) + need.shape, f32),
            pltpu.VMEM((writers - 1, n_z) + need.shape, f32),
            dma((6,)),
            dma((6,)),
            dma((writers + n_z - 2,)),
            dma((writers + n_z - 2,)),
            dma,
        ],
        compiler_params=pltpu.CompilerParams(collective_id=1, has_side_effects=True),
        name="halo",
    )(velocity, y_faces, z_faces, need)

    table = jnp.asarray(split_table())
    outgoing, squares, meta = pl.pallas_call(
        blocks_kernel,
        out_shape=(
            jax.ShapeDtypeStruct((writers * region * comps, width), f32),
            jax.ShapeDtypeStruct((8, cells_z), f32),
            jax.ShapeDtypeStruct((writers * capacity,), jnp.int32),
        ),
        in_specs=[anywhere] * 2 + [vmem] * 3,
        out_specs=(vmem, vmem, smem),
        scratch_shapes=[
            pltpu.VMEM((nblk * comps, width), f32),
            pltpu.SMEM((3 * nblk,), jnp.int32),
            dma,
            dma,
        ],
        compiler_params=pltpu.CompilerParams(vmem_limit_bytes=48 * 2**20),
        name="blocks",
    )(
        plan.reshape(3 * nblk),
        jnp.zeros((writers * capacity,), jnp.int32),
        velocity,
        halos,
        table,
    )
    outgoing = outgoing.reshape(writers, region * comps, width)
    part = min(capacity, 128)
    meta = meta.reshape(writers, capacity // part, part)

    def exchange(index, outgoing, squares, meta):
        rows = tiers[index] * comps
        return pl.pallas_call(
            functools.partial(exchange_kernel, n_x, n_y, n_z, rows),
            out_shape=(
                jax.ShapeDtypeStruct(outgoing.shape, f32),
                jax.ShapeDtypeStruct(squares.shape, f32),
                jax.ShapeDtypeStruct(meta.shape, jnp.int32),
            ),
            in_specs=[anywhere, vmem, anywhere],
            out_specs=(anywhere, vmem, anywhere),
            scratch_shapes=[
                pltpu.VMEM((n_z,) + squares.shape, f32),
                pltpu.VMEM((writers - 1, n_z) + squares.shape, f32),
                dma((writers - 1,)),
                dma((writers - 1,)),
                dma((writers + n_z - 2,)),
                dma((writers + n_z - 2,)),
                dma((writers - 1,)),
                dma((writers - 1,)),
                dma((3,)),
            ],
            compiler_params=pltpu.CompilerParams(collective_id=2 + index, has_side_effects=True),
            name=f"exchange{tiers[index]}",
        )(outgoing, squares, meta)

    branches = [functools.partial(exchange, index) for index in range(len(tiers))]
    arrived, squares, heard = lax.switch(tier[0], branches, outgoing, squares, meta)

    every = velocity.size * n_x * n_y * n_z
    received = pl.pallas_call(
        functools.partial(unpack_kernel, float(every)),
        grid=(writers,),
        in_specs=[
            smem,
            pl.BlockSpec((8, cells_z), lambda s: (0, 0)),
            pl.BlockSpec((1, region * comps, width), lambda s: (s, 0, 0)),
        ],
        out_specs=pl.BlockSpec((comps, 1, capacity, width), lambda s: (0, s, 0, 0)),
        out_shape=jax.ShapeDtypeStruct((comps, writers, capacity, width), f32),
        scratch_shapes=[pltpu.VMEM((8, width), f32)],
        name="unpack",
    )(heard.reshape(writers * capacity), squares, arrived)
    return received.reshape(1, 1, comps, writers, capacity, width)


def solution(mesh):
    return jax.shard_map(
        local,
        mesh=mesh,
        in_specs=(
            P(None, "gx", "gy", "wa"),
            P("gx", "gy", "wa", None),
            P("gx", "gy", "wa", None, None),
        ),
        out_specs=P(("gx", "gy"), "wa", None, None, None, None),
        check_vma=False,
    )
```

```python
import functools
import math

import jax
import jax.numpy as jnp
import numpy as np
from jax import lax
from jax.experimental import pallas as pl
from jax.experimental.pallas import tpu as pltpu
from jax.sharding import PartitionSpec as P

BY = 8
BZ = 16
UNROLL = 2
MESH = pl.DeviceIdType.MESH


def dct_table(count):
    freqs, points = np.arange(count)[:, None], np.arange(count)[None, :]
    table = np.cos(np.pi * (points + 0.5) * freqs / count) * np.sqrt(2.0 / count)
    return np.where(freqs == 0, table * np.sqrt(0.5), table)


def split_table():
    kron = np.kron(dct_table(BY), dct_table(BZ)).T.astype(np.float32)
    high = kron.astype(jnp.bfloat16)
    low = (kron - high.astype(np.float32)).astype(jnp.bfloat16)
    return np.block([[high, low], [high, np.zeros_like(low)]]).astype(jnp.bfloat16)


def spill_tiles(used, direct):
    return lax.shift_right_logical(jnp.maximum(used - direct, 0) + 7, 3)


def faces_kernel(
    writers, capacity, region, direct, n_y, targets, lens, vel, plan, counts, y_faces, z_faces, need,
    sums
):
    comps, cells_x, cells_y, cells_z = vel.shape
    lane = lax.broadcasted_iota(jnp.int32, (cells_y, cells_z), 1)

    def plane(x, acc):
        here = lane == x
        rolled = [
            pltpu.roll(vel[comp, x], lax.rem(x + last, cells_z), 1)
            for last in range(2)
            for comp in (0, 1)
        ]
        for i, comp in enumerate((0, 2)):
            y_faces[0, i, pl.ds(x, 1), :] = vel[comp, x, 0:1]
            y_faces[1, i, pl.ds(x, 1), :] = vel[comp, x, cells_y - 1 : cells_y]
        return tuple(jnp.where(here, new, old) for new, old in zip(rolled, acc))

    zero = jnp.zeros((cells_y, cells_z), jnp.float32)
    columns = lax.fori_loop(0, cells_x, plane, (zero,) * 4, unroll=4)
    for last in range(2):
        for i in range(2):
            z_faces[last, i] = columns[2 * last + i]

    t, kept = targets[...], lens[...]
    rows, lanes = t.shape
    shape = (lanes, lanes)
    upper = (
        lax.broadcasted_iota(jnp.int32, shape, 0) < lax.broadcasted_iota(jnp.int32, shape, 1)
    ).astype(jnp.float32).astype(jnp.bfloat16)
    square = (rows, rows)
    lower = (
        lax.broadcasted_iota(jnp.int32, square, 1) < lax.broadcasted_iota(jnp.int32, square, 0)
    ).astype(jnp.float32).astype(jnp.bfloat16)
    weight = kept.astype(jnp.float32)

    def body(w, acc):
        spot, start, site = acc
        mine = t == w
        ones = mine.astype(jnp.float32)
        sizes = jnp.where(mine, weight, 0.0)
        both = jnp.concatenate([ones, sizes], axis=0).astype(jnp.bfloat16)
        sums[pl.ds(w, 1), :] = jnp.sum(sizes, axis=0, keepdims=True)
        inner = jnp.dot(both, upper, preferred_element_type=jnp.float32)
        side = jnp.concatenate([ones, sizes], axis=1).astype(jnp.bfloat16)
        before = jnp.dot(lower, side, preferred_element_type=jnp.float32)
        rank = inner[:rows] + jnp.sum(before[:, :lanes], axis=1, keepdims=True)
        offset = inner[rows:] + jnp.sum(before[:, lanes:], axis=1, keepdims=True)
        spot = jnp.where(mine, w * capacity + rank.astype(jnp.int32), spot)
        offset = offset.astype(jnp.int32)
        start = jnp.where(mine, offset, start)
        site = jnp.where(mine, w * region, site)
        return spot, start, site

    none = jnp.zeros_like(t)
    spot, start, site = lax.fori_loop(0, writers, body, (none, none, none), unroll=8)
    shift = start & (lanes - 1)
    row = lax.shift_right_logical(start, lanes.bit_length() - 1)
    plan[2] = spot
    plan[0] = (row + site) * (comps << 16) + shift
    plan[1] = row * (comps << 16) + (lanes - shift) * 256 + kept
    used = jnp.sum(sums[...], axis=1, keepdims=True).astype(jnp.int32)
    used = jnp.broadcast_to(lax.shift_right_logical(used + (lanes - 1), 7), counts.shape)
    counts[...] = used
    writer = lax.broadcasted_iota(jnp.int32, counts.shape, 0)
    half = max(1, n_y // 2)
    far_side = lax.div(lax.rem(writer, n_y), half) != lax.div(lax.axis_index("gy"), half)
    over = jnp.where(far_side, spill_tiles(used, direct) * 8, 0)
    most = jnp.max(used.astype(jnp.float32), axis=0, keepdims=True)
    extra = jnp.sum(over.astype(jnp.float32), axis=0, keepdims=True)
    line = lax.broadcasted_iota(jnp.int32, need.shape, 0)
    need[...] = jnp.where(line == 0, most, jnp.where(line == 1, extra, 0.0))


def plane_offsets(n_x, n_y):
    offsets = [(i, j) for i in range(n_x) for j in range(n_y) if i or j]
    return sorted(offsets, key=lambda o: (bool(o[0]) and bool(o[1]), min(o[1], n_y - o[1])))


def plane_peers(n_x, n_y):
    a, b, c = (lax.axis_index(axis) for axis in ("gx", "gy", "wa"))
    return [(lax.rem(a + i, n_x), lax.rem(b + j, n_y), c) for i, j in plane_offsets(n_x, n_y)]


def line_mates(n_z):
    a, b, c = (lax.axis_index(axis) for axis in ("gx", "gy", "wa"))
    return [(a, b, lax.rem(c + k, n_z)) for k in range(1, n_z)]


def send_to(src, dst, send_sem, recv_sem, device):
    copy = pltpu.make_async_remote_copy(
        src_ref=src,
        dst_ref=dst,
        send_sem=send_sem,
        recv_sem=recv_sem,
        device_id=device,
        device_id_type=MESH,
    )
    copy.start()
    return copy


def halo_kernel(
    sizes, tiers, vel, y_faces, z_faces, need, halos, tier, near, far, send_sem, recv_sem, part_send,
    part_recv, own_sem,
):
    place = [lax.axis_index(axis) for axis in ("gx", "gy", "wa")]
    n_x, n_y, n_z = sizes
    cells_x = vel.shape[1]

    def beside(axis, step):
        size = sizes[axis]
        moved = lax.rem(place[axis] + step + size, size)
        return tuple(moved if i == axis else p for i, p in enumerate(place))

    across, along = pl.ds(0, vel.shape[2]), pl.ds(0, cells_x)
    moves = [
        (vel.at[pl.ds(1, 2), cells_x - 1], halos.at[0, :, across], beside(0, 1)),
        (vel.at[pl.ds(1, 2), 0], halos.at[1, :, across], beside(0, -1)),
        (y_faces.at[1], halos.at[2, :, along], beside(1, 1)),
        (y_faces.at[0], halos.at[3, :, along], beside(1, -1)),
        (z_faces.at[1], halos.at[4, :, across], beside(2, 1)),
        (z_faces.at[0], halos.at[5, :, across], beside(2, -1)),
    ]
    peers, mates = plane_peers(n_x, n_y), line_mates(n_z)
    others = [device for _, _, device in moves] + peers + mates
    barrier = pltpu.get_barrier_semaphore()
    for device in others:
        pl.semaphore_signal(barrier, inc=1, device_id=device, device_id_type=MESH)
    pl.semaphore_wait(barrier, len(others))
    c = place[2]
    own = pltpu.make_async_copy(need, near.at[c], own_sem)
    own.start()
    first = [
        send_to(need, near.at[c], part_send.at[k], part_recv.at[k], device)
        for k, device in enumerate(mates)
    ]
    copies = [
        send_to(src, dst, send_sem.at[k], recv_sem.at[k], device)
        for k, (src, dst, device) in enumerate(moves)
    ]
    own.wait()
    for copy in first:
        copy.wait()
    for k, device in enumerate(peers):
        sem = n_z - 1 + k
        copies.append(send_to(near, far.at[k], part_send.at[sem], part_recv.at[sem], device))
    for copy in copies:
        copy.wait()
    most = jnp.maximum(jnp.max(near[...], axis=0), jnp.max(far[...], axis=(0, 1)))
    pair, extra = jnp.max(most[0:1]), jnp.max(most[1:2])
    chosen = jnp.int32(len(tiers) - 1)
    for index in reversed(range(len(tiers) - 1)):
        rows, spill = tiers[index]
        fits = pair <= rows
        if spill:
            fits = jnp.logical_and(fits, extra <= spill)
        chosen = jnp.where(fits, index, chosen)
    tier[0] = chosen


def block_rows(plane):
    cells_y, cells_z = plane.shape
    tiles = plane.reshape(cells_y // BY, BY, cells_z)
    sub = lax.broadcasted_iota(jnp.int32, tiles.shape, 1)
    group = lax.broadcasted_iota(jnp.int32, tiles.shape, 2) // BZ
    k = 1
    while k < BY:
        s_bit, g_bit = (sub & k) != 0, (group & k) != 0
        fwd = pltpu.roll(pltpu.roll(tiles, BY - k, 1), k * BZ, 2)
        back = pltpu.roll(pltpu.roll(tiles, k, 1), cells_z - k * BZ, 2)
        tiles = jnp.where(s_bit == g_bit, tiles, jnp.where(g_bit, fwd, back))
        k *= 2
    return tiles.reshape(cells_y, cells_z)


def blocks_kernel(
    n_x, n_y, region, direct, lists, tallies, blank, vel, halos, table, out, squares, meta, spill,
    starts, coeffs, plan, counts, meta_sem, plan_sem, count_sem,
):
    comps, cells_x, cells_y, cells_z = vel.shape
    nblk = coeffs.shape[0] // comps
    per_plane = nblk // cells_x
    width = out.shape[1]
    row = lax.broadcasted_iota(jnp.int32, (cells_y, cells_z), 0)
    lane = lax.broadcasted_iota(jnp.int32, (cells_y, cells_z), 1)
    clear = pltpu.make_async_copy(blank, meta, meta_sem)
    clear.start()
    fetch = pltpu.make_async_copy(lists, plan, plan_sem)
    fetch.start()
    tally = pltpu.make_async_copy(tallies, counts, count_sem)
    tally.start()

    def plane(x, acc):
        u, v, w = vel[0, x], vel[1, x], vel[2, x]

        def along_x(comp):
            nxt = jnp.where(
                x == cells_x - 1, halos[1, comp - 1, :cells_y], vel[comp, jnp.minimum(x + 1, cells_x - 1)]
            )
            prv = jnp.where(x == 0, halos[0, comp - 1, :cells_y], vel[comp, jnp.maximum(x - 1, 0)])
            return (nxt - prv) * 0.5

        def along_y(f, face):
            nxt = jnp.where(
                row == cells_y - 1, halos[3, face, pl.ds(x, 1), :], pltpu.roll(f, cells_y - 1, 0)
            )
            prv = jnp.where(row == 0, halos[2, face, pl.ds(x, 1), :], pltpu.roll(f, 1, 0))
            return (nxt - prv) * 0.5

        def along_z(f, face):
            after = pltpu.roll(halos[5, face, :cells_y], cells_z - 1 - x, 1)
            before = pltpu.roll(halos[4, face, :cells_y], lax.rem(cells_z - x, cells_z), 1)
            nxt = jnp.where(lane == cells_z - 1, after, pltpu.roll(f, cells_z - 1, 1))
            prv = jnp.where(lane == 0, before, pltpu.roll(f, 1, 1))
            return (nxt - prv) * 0.5

        curl = (
            along_y(w, 1) - along_z(v, 1),
            along_z(u, 0) - along_x(2),
            along_x(1) - along_y(u, 0),
        )
        for c in curl:
            acc = acc + jnp.sum((c * c).reshape(cells_y // 8, 8, cells_z), axis=0)
        flat = jnp.concatenate([block_rows(c) for c in curl], axis=0)
        high = flat.astype(jnp.bfloat16)
        low = (flat - high.astype(jnp.float32)).astype(jnp.bfloat16)
        both = jnp.dot(
            jnp.concatenate([high, low], axis=1), table[...], preferred_element_type=jnp.float32
        )
        result = both[:, :width] + both[:, width:]
        start = x * (comps * per_plane)
        for c in range(comps):
            coeffs[pl.ds(start + c, per_plane, stride=comps), :] = result[
                c * per_plane : (c + 1) * per_plane
            ]
        return acc

    spread = lax.broadcasted_iota(jnp.int32, (comps, width), 1)
    group = 8

    def place(x):
        for start in range(0, per_plane, group):
            found = []
            for k in range(start, min(start + group, per_plane)):
                i = x * per_plane + k
                word = plan[i]
                meta[plan[2 * nblk + i]] = plan[nblk + i]
                shift = word & (width - 1)
                row = lax.shift_right_logical(word, 16)
                moved = pltpu.roll(coeffs[pl.ds(i * comps, comps), :], shift, 1)
                found.append((row, moved, spread >= shift))
            for row, moved, mask in found:
                pltpu.store(out.at[pl.ds(row, comps), :], moved, mask=mask)
                out[pl.ds(row + comps, comps), :] = moved

    together = next(n for n in (UNROLL, 2, 1) if cells_x % n == 0)

    def step(t, acc):
        for k in range(together):
            place((t - 1) * together + k)
        return planes(t, acc)

    def planes(t, acc):
        for k in range(together):
            acc = plane(t * together + k, acc)
        return acc

    clear.wait()
    fetch.wait()
    tally.wait()
    first = planes(0, jnp.zeros((8, cells_z), jnp.float32))
    squares[...] = lax.fori_loop(1, cells_x // together, step, first)
    for k in range(together):
        place(cells_x - together + k)

    half = max(1, n_y // 2)
    facing = lax.rem(lax.div(lax.axis_index("gy"), half) + 1, 2) * half
    most = spill.shape[0] // comps

    def segment(j, begin):
        writer = lax.div(j, half) * n_y + facing + lax.rem(j, half)
        tiles = jnp.minimum(spill_tiles(counts[writer, 0], direct), most - begin)
        starts[j] = begin
        source = (writer * region + direct) * comps

        def tile(i, _):
            for c in range(comps):
                at = source + (i * comps + c) * 8
                spill[(begin + i) * comps + c] = out[pl.ds(pl.multiple_of(at, 8), 8), :]
            return 0

        lax.fori_loop(0, tiles, tile, 0)
        return begin + tiles

    lax.fori_loop(0, n_x * half, segment, jnp.int32(0))


def exchange_kernel(
    n_x, n_y, n_z, comps, rows, direct, extra, send, squares, meta, spill, starts, recv, total, heard,
    near, far, send_sem, recv_sem, part_send, part_recv, word_send, word_recv, own_sem, *relay,
):
    a, b = lax.axis_index("gx"), lax.axis_index("gy")
    c = lax.axis_index("wa")
    me = a * n_y + b
    half = max(1, n_y // 2)
    peers, mates = plane_peers(n_x, n_y), line_mates(n_z)
    barrier = pltpu.get_barrier_semaphore()
    for device in mates + peers:
        pl.semaphore_signal(barrier, inc=1, device_id=device, device_id_type=MESH)
    pl.semaphore_wait(barrier, len(peers) + len(mates))

    own = [
        pltpu.make_async_copy(squares, near.at[c], own_sem.at[0]),
        pltpu.make_async_copy(meta.at[me], heard.at[me], own_sem.at[1]),
        pltpu.make_async_copy(
            send.at[me, pl.ds(0, rows * comps)], recv.at[me, pl.ds(0, rows * comps)], own_sem.at[2]
        ),
    ]
    for copy in own:
        copy.start()
    copies, relays = [], []
    if extra:
        (
            landed, ready, begins, marks, relay_send, relay_recv, spill_send, spill_recv, begin_sem
        ) = relay
        partner = (a, lax.rem(b + half, n_y), c)
        relays = [
            send_to(starts, begins, spill_send.at[0], spill_recv.at[0], partner),
            send_to(
                spill.at[pl.ds(0, extra * comps // 8)],
                landed.at[pl.ds(0, extra * comps // 8)],
                spill_send.at[1],
                spill_recv.at[1],
                partner,
            ),
        ]
    first = [
        send_to(squares, near.at[c], part_send.at[k], part_recv.at[k], device)
        for k, device in enumerate(mates)
    ]

    def number(device):
        return device[0] * n_y + device[1]

    offsets = plane_offsets(n_x, n_y)

    def blocks_to(k):
        device = peers[k]

        def go(size):
            used = pl.ds(0, size * comps)
            return pltpu.make_async_remote_copy(
                src_ref=send.at[number(device), used],
                dst_ref=recv.at[me, used],
                send_sem=send_sem.at[k],
                recv_sem=recv_sem.at[k],
                device_id=device,
                device_id_type=MESH,
            )

        if not extra:
            copy = go(rows)
            copy.start()
            return [copy.wait]
        crosses = lax.div(device[1], half) != lax.div(b, half)
        inward = lax.div(lax.rem(b - offsets[k][1] + n_y, n_y), half) != lax.div(b, half)

        @pl.when(crosses)
        def _():
            go(direct).start()

        @pl.when(jnp.logical_not(crosses))
        def _():
            go(rows).start()

        def wait():
            @pl.when(crosses)
            def _():
                go(direct).wait_send()

            @pl.when(jnp.logical_not(crosses))
            def _():
                go(rows).wait_send()

            @pl.when(inward)
            def _():
                go(direct).wait_recv()

            @pl.when(jnp.logical_not(inward))
            def _():
                go(rows).wait_recv()

        return [wait]

    waits = []
    for k, device in enumerate(peers):
        copies.append(
            send_to(meta.at[number(device)], heard.at[me], word_send.at[k], word_recv.at[k], device)
        )
    ahead = min(3, len(peers))
    for k in range(ahead):
        waits += blocks_to(k)
    own[0].wait()
    for copy in first:
        copy.wait()
    for k, device in enumerate(peers):
        sem = n_z - 1 + k
        copies.append(send_to(near, far.at[k], part_send.at[sem], part_recv.at[sem], device))
    for k in range(ahead, len(peers)):
        waits += blocks_to(k)
    if extra:
        relays[0].wait()
        load = pltpu.make_async_copy(begins, marks, begin_sem.at[0])
        load.start()
        load.wait()
        relays[1].wait()
        size = (rows - direct) * comps
        source = a * n_y + lax.rem(b + half, n_y)
        mine = lax.rem(b, half)
        base = b - mine
        places = [
            (lax.rem(a + i, n_x), lax.rem(mine + j, half)) for i in range(n_x) for j in range(half)
        ]
        for k, (x, y) in enumerate(places):
            begin = marks[0, x * half + y] * comps

            def tile(i, _, k=k, begin=begin):
                ready[k, pl.ds(pl.multiple_of(i * 8, 8), 8), :] = landed[begin + i]
                return 0

            lax.fori_loop(0, size // 8, tile, 0)
        spot = recv.at[source, pl.ds(direct * comps, size)]
        for k, (x, y) in enumerate(places):
            if k:
                copies.append(
                    send_to(ready.at[k], spot, relay_send.at[k], relay_recv.at[k], (x, base + y, c))
                )
        keep = pltpu.make_async_copy(ready.at[0], spot, begin_sem.at[1])
        keep.start()
        keep.wait()
    for copy in own[1:]:
        copy.wait()
    for copy in copies:
        copy.wait()
    for wait in waits:
        wait()
    total[...] = jnp.sum(near[...], axis=0) + jnp.sum(far[...], axis=(0, 1))


def unpack_kernel(every, meta, squares, recv, out, scale):
    comps, _, capacity, width = out.shape
    source = pl.program_id(0)

    @pl.when(source == 0)
    def _():
        total = jnp.sum(squares[...], keepdims=True)
        scale[...] = jnp.broadcast_to(1.0 / jnp.sqrt(total / every + 1e-06), scale.shape)

    lane = lax.broadcasted_iota(jnp.int32, (comps, width), 1)
    factor = scale[:comps]
    group = math.gcd(capacity, 32)
    first = source * capacity

    def some(t, _):
        start = first + t * group
        for k in range(group):
            mark = meta[start + k]
            fields = jnp.full((comps, width), mark, jnp.int32)
            ahead = lane + (lax.shift_right_logical(fields, 8) & 255)
            row = lax.shift_right_logical(mark, 16)
            head = recv[0, pl.ds(row, comps), :]
            tail = recv[0, pl.ds(row + comps, comps), :]
            joined = jnp.where(ahead >= width, head, tail)
            moved = pltpu.roll(joined, lax.shift_right_logical(mark, 8) & (width - 1), 1)
            value = jnp.where(lane < (fields & 255), moved * factor, 0.0)
            for c in range(comps):
                out[c, 0, pl.ds(t * group + k, 1), :] = value[c : c + 1]
        return 0

    lax.fori_loop(0, capacity // group, some, 0)


def tier_sizes(capacity, n_y):
    def up(part):
        return -(-capacity * part // (64 * 8)) * 8

    direct = [(up(part), 0) for part in (48, 56, 64)]
    if n_y % 2:
        return up(64), direct
    parts = ((38, 28), (38, 32), (39, 36), (40, 44), (44, 52))
    spilled = [(up(rows), up(extra)) for rows, extra in parts]
    return up(18), spilled + direct


def local(velocity, lengths, destinations):
    n_x, n_y, n_z = lax.axis_size("gx"), lax.axis_size("gy"), lax.axis_size("wa")
    comps, cells_x, cells_y, cells_z = velocity.shape
    width = BY * BZ
    nblk = cells_x * cells_y * cells_z // width
    writers = n_x * n_y
    capacity = max(2, 2 * nblk // writers)
    region = capacity + 8
    f32 = jnp.float32
    direct, tiers = tier_sizes(capacity, n_y)
    most_extra = max([8] + [extra for _, extra in tiers])
    senders = n_x * max(1, n_y // 2)

    smem = pl.BlockSpec(memory_space=pltpu.SMEM)
    vmem = pl.BlockSpec(memory_space=pltpu.VMEM)
    anywhere = pl.BlockSpec(memory_space=pl.ANY)
    dma = pltpu.SemaphoreType.DMA
    plan, tallies, y_faces, z_faces, need = pl.pallas_call(
        functools.partial(faces_kernel, writers, capacity, region, direct, n_y),
        out_shape=(
            jax.ShapeDtypeStruct((3, nblk // 128, 128), jnp.int32),
            jax.ShapeDtypeStruct((writers, 128), jnp.int32),
            jax.ShapeDtypeStruct((2, 2, cells_x, cells_z), f32),
            jax.ShapeDtypeStruct((2, 2, cells_y, cells_z), f32),
            jax.ShapeDtypeStruct((8, 128), f32),
        ),
        scratch_shapes=[pltpu.VMEM((writers, 128), f32)],
        name="faces",
    )(destinations.reshape(nblk // 128, 128), lengths.reshape(nblk // 128, 128), velocity)
    halos, tier = pl.pallas_call(
        functools.partial(halo_kernel, (n_x, n_y, n_z), tiers),
        out_shape=(
            jax.ShapeDtypeStruct((6, 2, max(cells_x, cells_y), cells_z), f32),
            jax.ShapeDtypeStruct((1,), jnp.int32),
        ),
        in_specs=[anywhere] * 3 + [vmem],
        out_specs=(anywhere, smem),
        scratch_shapes=[
            pltpu.VMEM((n_z,) + need.shape, f32),
            pltpu.VMEM((writers - 1, n_z) + need.shape, f32),
            dma((6,)),
            dma((6,)),
            dma((writers + n_z - 2,)),
            dma((writers + n_z - 2,)),
            dma,
        ],
        compiler_params=pltpu.CompilerParams(collective_id=1, has_side_effects=True),
        name="halo",
    )(velocity, y_faces, z_faces, need)

    table = jnp.asarray(split_table())
    outgoing, squares, meta, spill, starts = pl.pallas_call(
        functools.partial(blocks_kernel, n_x, n_y, region, direct),
        out_shape=(
            jax.ShapeDtypeStruct((writers * region * comps, width), f32),
            jax.ShapeDtypeStruct((8, cells_z), f32),
            jax.ShapeDtypeStruct((writers * capacity,), jnp.int32),
            jax.ShapeDtypeStruct((most_extra * comps // 8, 8, width), f32),
            jax.ShapeDtypeStruct((128,), jnp.int32),
        ),
        in_specs=[anywhere] * 3 + [vmem] * 3,
        out_specs=(vmem, vmem, smem, vmem, smem),
        scratch_shapes=[
            pltpu.VMEM((nblk * comps, width), f32),
            pltpu.SMEM((3 * nblk,), jnp.int32),
            pltpu.SMEM((writers, 128), jnp.int32),
            dma,
            dma,
            dma,
        ],
        compiler_params=pltpu.CompilerParams(vmem_limit_bytes=48 * 2**20),
        name="blocks",
    )(
        plan.reshape(3 * nblk),
        tallies,
        jnp.zeros((writers * capacity,), jnp.int32),
        velocity,
        halos,
        table,
    )
    outgoing = outgoing.reshape(writers, region * comps, width)
    part = min(capacity, 128)
    meta = meta.reshape(writers, capacity // part, part)

    def exchange(index, *operands):
        rows, extra = tiers[index]
        size = (rows - direct) * comps
        relay = [
            pltpu.VMEM(((extra * comps + size) // 8, 8, width), f32),
            pltpu.VMEM((senders, size, width), f32),
            pltpu.VMEM((1, 128), jnp.int32),
            pltpu.SMEM((1, 128), jnp.int32),
            dma((senders,)),
            dma((senders,)),
            dma((2,)),
            dma((2,)),
            dma((2,)),
        ]
        return pl.pallas_call(
            functools.partial(exchange_kernel, n_x, n_y, n_z, comps, rows, direct, extra),
            out_shape=(
                jax.ShapeDtypeStruct(outgoing.shape, f32),
                jax.ShapeDtypeStruct(squares.shape, f32),
                jax.ShapeDtypeStruct(meta.shape, jnp.int32),
            ),
            in_specs=[anywhere, vmem, anywhere, anywhere, anywhere],
            out_specs=(anywhere, vmem, anywhere),
            scratch_shapes=[
                pltpu.VMEM((n_z,) + squares.shape, f32),
                pltpu.VMEM((writers - 1, n_z) + squares.shape, f32),
                dma((writers - 1,)),
                dma((writers - 1,)),
                dma((writers + n_z - 2,)),
                dma((writers + n_z - 2,)),
                dma((writers - 1,)),
                dma((writers - 1,)),
                dma((3,)),
            ]
            + (relay if extra else []),
            compiler_params=pltpu.CompilerParams(collective_id=2 + index, has_side_effects=True),
            name=f"exchange{rows}_{extra}",
        )(*operands)

    branches = [functools.partial(exchange, index) for index in range(len(tiers))]
    arrived, squares, heard = lax.switch(
        tier[0], branches, outgoing, squares, meta, spill, starts.reshape(1, 128)
    )

    every = velocity.size * n_x * n_y * n_z
    received = pl.pallas_call(
        functools.partial(unpack_kernel, float(every)),
        grid=(writers,),
        in_specs=[
            smem,
            pl.BlockSpec((8, cells_z), lambda s: (0, 0)),
            pl.BlockSpec((1, region * comps, width), lambda s: (s, 0, 0)),
        ],
        out_specs=pl.BlockSpec((comps, 1, capacity, width), lambda s: (0, s, 0, 0)),
        out_shape=jax.ShapeDtypeStruct((comps, writers, capacity, width), f32),
        scratch_shapes=[pltpu.VMEM((8, width), f32)],
        name="unpack",
    )(heard.reshape(writers * capacity), squares, arrived)
    return received.reshape(1, 1, comps, writers, capacity, width)


def solution(mesh):
    return jax.shard_map(
        local,
        mesh=mesh,
        in_specs=(
            P(None, "gx", "gy", "wa"),
            P("gx", "gy", "wa", None),
            P("gx", "gy", "wa", None, None),
        ),
        out_specs=P(("gx", "gy"), "wa", None, None, None, None),
        check_vma=False,
    )
```

```python
import functools
import math

import jax
import jax.numpy as jnp
import numpy as np
from jax import lax
from jax.experimental import pallas as pl
from jax.experimental.pallas import tpu as pltpu
from jax.sharding import PartitionSpec as P

BY = 8
BZ = 16
UNROLL = 2
MESH = pl.DeviceIdType.MESH


def dct_table(count):
    freqs, points = np.arange(count)[:, None], np.arange(count)[None, :]
    table = np.cos(np.pi * (points + 0.5) * freqs / count) * np.sqrt(2.0 / count)
    return np.where(freqs == 0, table * np.sqrt(0.5), table)


def split_table():
    kron = np.kron(dct_table(BY), dct_table(BZ)).T.astype(np.float32)
    high = kron.astype(jnp.bfloat16)
    low = (kron - high.astype(np.float32)).astype(jnp.bfloat16)
    return np.block([[high, low], [high, np.zeros_like(low)]]).astype(jnp.bfloat16)


def spill_tiles(used, direct):
    return lax.shift_right_logical(jnp.maximum(used - direct, 0) + 7, 3)


def faces_kernel(
    writers, capacity, region, direct, n_y, targets, lens, vel, plan, counts, y_faces, z_faces, need,
    sums
):
    comps, cells_x, cells_y, cells_z = vel.shape
    lane = lax.broadcasted_iota(jnp.int32, (cells_y, cells_z), 1)

    def plane(x, acc):
        here = lane == x
        rolled = [
            pltpu.roll(vel[comp, x], lax.rem(x + last, cells_z), 1)
            for last in range(2)
            for comp in (0, 1)
        ]
        for i, comp in enumerate((0, 2)):
            y_faces[0, i, pl.ds(x, 1), :] = vel[comp, x, 0:1]
            y_faces[1, i, pl.ds(x, 1), :] = vel[comp, x, cells_y - 1 : cells_y]
        return tuple(jnp.where(here, new, old) for new, old in zip(rolled, acc))

    zero = jnp.zeros((cells_y, cells_z), jnp.float32)
    columns = lax.fori_loop(0, cells_x, plane, (zero,) * 4, unroll=4)
    for last in range(2):
        for i in range(2):
            z_faces[last, i] = columns[2 * last + i]

    t, kept = targets[...], lens[...]
    rows, lanes = t.shape
    shape = (lanes, lanes)
    upper = (
        lax.broadcasted_iota(jnp.int32, shape, 0) < lax.broadcasted_iota(jnp.int32, shape, 1)
    ).astype(jnp.float32).astype(jnp.bfloat16)
    square = (rows, rows)
    lower = (
        lax.broadcasted_iota(jnp.int32, square, 1) < lax.broadcasted_iota(jnp.int32, square, 0)
    ).astype(jnp.float32).astype(jnp.bfloat16)
    weight = kept.astype(jnp.float32)

    def body(w, acc):
        spot, start, site = acc
        mine = t == w
        ones = mine.astype(jnp.float32)
        sizes = jnp.where(mine, weight, 0.0)
        both = jnp.concatenate([ones, sizes], axis=0).astype(jnp.bfloat16)
        sums[pl.ds(w, 1), :] = jnp.sum(sizes, axis=0, keepdims=True)
        inner = jnp.dot(both, upper, preferred_element_type=jnp.float32)
        side = jnp.concatenate([ones, sizes], axis=1).astype(jnp.bfloat16)
        before = jnp.dot(lower, side, preferred_element_type=jnp.float32)
        rank = inner[:rows] + jnp.sum(before[:, :lanes], axis=1, keepdims=True)
        offset = inner[rows:] + jnp.sum(before[:, lanes:], axis=1, keepdims=True)
        spot = jnp.where(mine, w * capacity + rank.astype(jnp.int32), spot)
        offset = offset.astype(jnp.int32)
        start = jnp.where(mine, offset, start)
        site = jnp.where(mine, w * region, site)
        return spot, start, site

    none = jnp.zeros_like(t)
    spot, start, site = lax.fori_loop(0, writers, body, (none, none, none), unroll=8)
    shift = start & (lanes - 1)
    row = lax.shift_right_logical(start, lanes.bit_length() - 1)
    plan[2] = spot
    plan[0] = (row + site) * (comps << 16) + shift
    plan[1] = row * (comps << 16) + (lanes - shift) * 256 + kept
    used = jnp.sum(sums[...], axis=1, keepdims=True).astype(jnp.int32)
    used = jnp.broadcast_to(lax.shift_right_logical(used + (lanes - 1), 7), counts.shape)
    counts[...] = used
    writer = lax.broadcasted_iota(jnp.int32, counts.shape, 0)
    half = max(1, n_y // 2)
    far_side = lax.div(lax.rem(writer, n_y), half) != lax.div(lax.axis_index("gy"), half)
    over = jnp.where(far_side, spill_tiles(used, direct) * 8, 0)
    most = jnp.max(used.astype(jnp.float32), axis=0, keepdims=True)
    extra = jnp.sum(over.astype(jnp.float32), axis=0, keepdims=True)
    line = lax.broadcasted_iota(jnp.int32, need.shape, 0)
    need[...] = jnp.where(line == 0, most, jnp.where(line == 1, extra, 0.0))


def plane_offsets(n_x, n_y):
    offsets = [(i, j) for i in range(n_x) for j in range(n_y) if i or j]
    return sorted(offsets, key=lambda o: (bool(o[0]) and bool(o[1]), min(o[1], n_y - o[1])))


def plane_peers(n_x, n_y):
    a, b, c = (lax.axis_index(axis) for axis in ("gx", "gy", "wa"))
    return [(lax.rem(a + i, n_x), lax.rem(b + j, n_y), c) for i, j in plane_offsets(n_x, n_y)]


def line_mates(n_z):
    a, b, c = (lax.axis_index(axis) for axis in ("gx", "gy", "wa"))
    return [(a, b, lax.rem(c + k, n_z)) for k in range(1, n_z)]


def send_to(src, dst, send_sem, recv_sem, device):
    copy = pltpu.make_async_remote_copy(
        src_ref=src,
        dst_ref=dst,
        send_sem=send_sem,
        recv_sem=recv_sem,
        device_id=device,
        device_id_type=MESH,
    )
    copy.start()
    return copy


def halo_kernel(
    sizes, tiers, vel, y_faces, z_faces, need, halos, tier, near, far, send_sem, recv_sem, part_send,
    part_recv, own_sem,
):
    place = [lax.axis_index(axis) for axis in ("gx", "gy", "wa")]
    n_x, n_y, n_z = sizes
    cells_x = vel.shape[1]

    def beside(axis, step):
        size = sizes[axis]
        moved = lax.rem(place[axis] + step + size, size)
        return tuple(moved if i == axis else p for i, p in enumerate(place))

    across, along = pl.ds(0, vel.shape[2]), pl.ds(0, cells_x)
    moves = [
        (vel.at[pl.ds(1, 2), cells_x - 1], halos.at[0, :, across], beside(0, 1)),
        (vel.at[pl.ds(1, 2), 0], halos.at[1, :, across], beside(0, -1)),
        (y_faces.at[1], halos.at[2, :, along], beside(1, 1)),
        (y_faces.at[0], halos.at[3, :, along], beside(1, -1)),
        (z_faces.at[1], halos.at[4, :, across], beside(2, 1)),
        (z_faces.at[0], halos.at[5, :, across], beside(2, -1)),
    ]
    peers, mates = plane_peers(n_x, n_y), line_mates(n_z)
    others = [device for _, _, device in moves] + peers + mates
    barrier = pltpu.get_barrier_semaphore()
    for device in others:
        pl.semaphore_signal(barrier, inc=1, device_id=device, device_id_type=MESH)
    pl.semaphore_wait(barrier, len(others))
    c = place[2]
    own = pltpu.make_async_copy(need, near.at[c], own_sem)
    own.start()
    first = [
        send_to(need, near.at[c], part_send.at[k], part_recv.at[k], device)
        for k, device in enumerate(mates)
    ]
    copies = [
        send_to(src, dst, send_sem.at[k], recv_sem.at[k], device)
        for k, (src, dst, device) in enumerate(moves)
    ]
    own.wait()
    for copy in first:
        copy.wait()
    for k, device in enumerate(peers):
        sem = n_z - 1 + k
        copies.append(send_to(near, far.at[k], part_send.at[sem], part_recv.at[sem], device))
    for copy in copies:
        copy.wait()
    most = jnp.maximum(jnp.max(near[...], axis=0), jnp.max(far[...], axis=(0, 1)))
    pair, extra = jnp.max(most[0:1]), jnp.max(most[1:2])
    chosen = jnp.int32(len(tiers) - 1)
    for index in reversed(range(len(tiers) - 1)):
        rows, spill = tiers[index]
        fits = pair <= rows
        if spill:
            fits = jnp.logical_and(fits, extra <= spill)
        chosen = jnp.where(fits, index, chosen)
    tier[0] = chosen


def block_rows(plane):
    cells_y, cells_z = plane.shape
    tiles = plane.reshape(cells_y // BY, BY, cells_z)
    sub = lax.broadcasted_iota(jnp.int32, tiles.shape, 1)
    group = lax.broadcasted_iota(jnp.int32, tiles.shape, 2) // BZ
    k = 1
    while k < BY:
        s_bit, g_bit = (sub & k) != 0, (group & k) != 0
        fwd = pltpu.roll(pltpu.roll(tiles, BY - k, 1), k * BZ, 2)
        back = pltpu.roll(pltpu.roll(tiles, k, 1), cells_z - k * BZ, 2)
        tiles = jnp.where(s_bit == g_bit, tiles, jnp.where(g_bit, fwd, back))
        k *= 2
    return tiles.reshape(cells_y, cells_z)


def blocks_kernel(
    n_x, n_y, region, direct, lists, tallies, blank, vel, halos, table, out, squares, meta, spill,
    starts, coeffs, plan, counts, meta_sem, plan_sem, count_sem,
):
    comps, cells_x, cells_y, cells_z = vel.shape
    nblk = coeffs.shape[0] // comps
    per_plane = nblk // cells_x
    width = out.shape[1]
    row = lax.broadcasted_iota(jnp.int32, (cells_y, cells_z), 0)
    lane = lax.broadcasted_iota(jnp.int32, (cells_y, cells_z), 1)
    clear = pltpu.make_async_copy(blank, meta, meta_sem)
    clear.start()
    fetch = pltpu.make_async_copy(lists, plan, plan_sem)
    fetch.start()
    tally = pltpu.make_async_copy(tallies, counts, count_sem)
    tally.start()

    def plane(x, acc):
        u, v, w = vel[0, x], vel[1, x], vel[2, x]

        def along_x(comp):
            nxt = jnp.where(
                x == cells_x - 1, halos[1, comp - 1, :cells_y], vel[comp, jnp.minimum(x + 1, cells_x - 1)]
            )
            prv = jnp.where(x == 0, halos[0, comp - 1, :cells_y], vel[comp, jnp.maximum(x - 1, 0)])
            return (nxt - prv) * 0.5

        def along_y(f, face):
            nxt = jnp.where(
                row == cells_y - 1, halos[3, face, pl.ds(x, 1), :], pltpu.roll(f, cells_y - 1, 0)
            )
            prv = jnp.where(row == 0, halos[2, face, pl.ds(x, 1), :], pltpu.roll(f, 1, 0))
            return (nxt - prv) * 0.5

        def along_z(f, face):
            after = pltpu.roll(halos[5, face, :cells_y], cells_z - 1 - x, 1)
            before = pltpu.roll(halos[4, face, :cells_y], lax.rem(cells_z - x, cells_z), 1)
            nxt = jnp.where(lane == cells_z - 1, after, pltpu.roll(f, cells_z - 1, 1))
            prv = jnp.where(lane == 0, before, pltpu.roll(f, 1, 1))
            return (nxt - prv) * 0.5

        curl = (
            along_y(w, 1) - along_z(v, 1),
            along_z(u, 0) - along_x(2),
            along_x(1) - along_y(u, 0),
        )
        for c in curl:
            acc = acc + jnp.sum((c * c).reshape(cells_y // 8, 8, cells_z), axis=0)
        flat = jnp.concatenate([block_rows(c) for c in curl], axis=0)
        high = flat.astype(jnp.bfloat16)
        low = (flat - high.astype(jnp.float32)).astype(jnp.bfloat16)
        both = jnp.dot(
            jnp.concatenate([high, low], axis=1), table[...], preferred_element_type=jnp.float32
        )
        result = both[:, :width] + both[:, width:]
        start = x * (comps * per_plane)
        for c in range(comps):
            coeffs[pl.ds(start + c, per_plane, stride=comps), :] = result[
                c * per_plane : (c + 1) * per_plane
            ]
        return acc

    spread = lax.broadcasted_iota(jnp.int32, (comps, width), 1)
    group = 8

    def place(x):
        for start in range(0, per_plane, group):
            found = []
            for k in range(start, min(start + group, per_plane)):
                i = x * per_plane + k
                word = plan[i]
                meta[plan[2 * nblk + i]] = plan[nblk + i]
                shift = word & (width - 1)
                row = lax.shift_right_logical(word, 16)
                moved = pltpu.roll(coeffs[pl.ds(i * comps, comps), :], shift, 1)
                found.append((row, moved, spread >= shift))
            for row, moved, mask in found:
                pltpu.store(out.at[pl.ds(row, comps), :], moved, mask=mask)
                out[pl.ds(row + comps, comps), :] = moved

    together = next(n for n in (UNROLL, 2, 1) if cells_x % n == 0)

    def step(t, acc):
        for k in range(together):
            place((t - 1) * together + k)
        return planes(t, acc)

    def planes(t, acc):
        for k in range(together):
            acc = plane(t * together + k, acc)
        return acc

    clear.wait()
    fetch.wait()
    tally.wait()
    first = planes(0, jnp.zeros((8, cells_z), jnp.float32))
    squares[...] = lax.fori_loop(1, cells_x // together, step, first)
    for k in range(together):
        place(cells_x - together + k)

    half = max(1, n_y // 2)
    facing = lax.rem(lax.div(lax.axis_index("gy"), half) + 1, 2) * half
    most = spill.shape[0] // comps

    def segment(j, begin):
        writer = lax.div(j, half) * n_y + facing + lax.rem(j, half)
        tiles = jnp.minimum(spill_tiles(counts[writer, 0], direct), most - begin)
        starts[j] = begin
        source = (writer * region + direct) * comps

        def tile(i, _):
            for c in range(comps):
                at = source + (i * comps + c) * 8
                spill[(begin + i) * comps + c] = out[pl.ds(pl.multiple_of(at, 8), 8), :]
            return 0

        lax.fori_loop(0, tiles, tile, 0)
        return begin + tiles

    lax.fori_loop(0, n_x * half, segment, jnp.int32(0))


def halves(n_y):
    return n_y if n_y % 2 else n_y // 2


def plane_order(n_x, n_y, sign):
    a, b, c = (lax.axis_index(axis) for axis in ("gx", "gy", "wa"))
    half = halves(n_y)
    mine = lax.rem(b, half)
    base = b - mine
    steps = [(i, j) for i in range(n_x) for j in range(half)]

    def at(base, i, j):
        x = lax.rem(a + sign * i + n_x, n_x)
        return (x, base + lax.rem(mine + sign * j + half, half), c)

    near = [at(base, i, j) for i, j in steps]
    other = lax.rem(base + half, n_y)
    far = [at(other, i, j) for i, j in steps] if half < n_y else []
    return near, far


def unpack(marks, source, target, lane, at):
    comps, width = lane.shape
    group = math.gcd(marks[0].shape[-1], 32)
    lists, k = marks
    per_line = lists.shape[2] // group

    def some(t, _):
        line = lax.div(t, per_line)
        start = lax.rem(t, per_line) * group
        for i in range(group):
            mark = lists[k, line, start + i]
            fields = jnp.full((comps, width), mark, jnp.int32)
            ahead = lane + (lax.shift_right_logical(fields, 8) & 255)
            row = lax.shift_right_logical(mark, 16)
            head = source[pl.ds(row, comps), :]
            tail = source[pl.ds(row + comps, comps), :]
            joined = jnp.where(ahead >= width, head, tail)
            moved = pltpu.roll(joined, lax.shift_right_logical(mark, 8) & (width - 1), 1)
            value = jnp.where(lane < (fields & 255), moved, 0.0)
            target[at, pl.ds((t * group + i) * comps, comps), :] = value
        return 0

    lax.fori_loop(0, lists.shape[1] * per_line, some, 0)


def exchange_kernel(
    n_x, n_y, n_z, comps, rows, direct, extra, send, squares, meta, spill, starts, recv, total, heard,
    done, near_part, far_part, stage, marks, send_sem, recv_sem, part_send, part_recv, word_send,
    word_recv, own_sem, done_sem, mark_sem, *rest,
):
    c = lax.axis_index("wa")
    near, far = plane_order(n_x, n_y, 1)
    me = near[0][0] * n_y + near[0][1]
    held, relay = rest[: len(near)], rest[len(near) :]
    peers, mates = near[1:] + far, line_mates(n_z)
    barrier = pltpu.get_barrier_semaphore()
    for device in mates + peers:
        pl.semaphore_signal(barrier, inc=1, device_id=device, device_id_type=MESH)
    pl.semaphore_wait(barrier, len(peers) + len(mates))

    def number(device):
        return device[0] * n_y + device[1]

    whole = pl.ds(0, rows * comps)
    own = [
        pltpu.make_async_copy(squares, near_part.at[c], own_sem.at[0]),
        pltpu.make_async_copy(meta.at[me], marks.at[0], mark_sem.at[0]),
        pltpu.make_async_copy(send.at[me, whole], held[0].at[whole], own_sem.at[1]),
    ]
    for copy in own:
        copy.start()
    first = [
        send_to(squares, near_part.at[c], part_send.at[k], part_recv.at[k], device)
        for k, device in enumerate(mates)
    ]
    relays, copies, words, blocks = [], [], [], []
    if extra:
        (
            landed, ready, begins, places, relay_send, relay_recv, spill_send, spill_recv, begin_sem
        ) = relay
        tiles = pl.ds(0, extra * comps // 8)
        relays = [
            send_to(starts, begins, spill_send.at[0], spill_recv.at[0], far[0]),
            send_to(spill.at[tiles], landed.at[tiles], spill_send.at[1], spill_recv.at[1], far[0]),
        ]
    for k, device in enumerate(peers):
        words.append(
            send_to(meta.at[number(device)], heard.at[k + 1], word_send.at[k], word_recv.at[k], device)
        )
    short = pl.ds(0, direct * comps) if extra else whole
    for k, device in enumerate(peers):
        if k + 1 < len(near):
            used, target = whole, held[k + 1].at[whole]
        else:
            used, target = short, recv.at[k + 1 - len(near), short]
        blocks.append(
            send_to(send.at[number(device), used], target, send_sem.at[k], recv_sem.at[k], device)
        )
    own[0].wait()
    for copy in first:
        copy.wait()
    for k, device in enumerate(peers):
        sem = n_z - 1 + k
        copies.append(
            send_to(near_part, far_part.at[k], part_send.at[sem], part_recv.at[sem], device)
        )
    if extra:
        relays[0].wait()
        load = pltpu.make_async_copy(begins, places, begin_sem.at[0])
        load.start()
        load.wait()
        relays[1].wait()
        size = (rows - direct) * comps
        half = halves(n_y)
        for k, (x, y, _) in enumerate(near):
            begin = places[0, x * half + lax.rem(y, half)] * comps

            def tile(i, _, k=k, begin=begin):
                ready[k, pl.ds(pl.multiple_of(i * 8, 8), 8), :] = landed[begin + i]
                return 0

            lax.fori_loop(0, size // 8, tile, 0)
        past = pl.ds(direct * comps, size)
        for k, device in enumerate(near):
            if k:
                copies.append(
                    send_to(
                        ready.at[k], recv.at[k, past], relay_send.at[k], relay_recv.at[k], device
                    )
                )
        keep = pltpu.make_async_copy(ready.at[0], recv.at[0, past], begin_sem.at[1])
        keep.start()
        keep.wait()
    lane = lax.broadcasted_iota(jnp.int32, (comps, send.shape[2]), 1)
    outs = []
    for k in range(len(near)):
        if k:
            words[k - 1].wait()
            load = pltpu.make_async_copy(heard.at[k], marks.at[k], mark_sem.at[k])
            load.start()
            load.wait()
            blocks[k - 1].wait()
        else:
            own[1].wait()
            own[2].wait()
        unpack((marks, k), held[k], stage, lane, k)
        out = pltpu.make_async_copy(stage.at[k], done.at[k], done_sem.at[k])
        out.start()
        outs.append(out)
    for copy in words[len(near) - 1 :] + blocks[len(near) - 1 :] + copies + outs:
        copy.wait()
    total[...] = jnp.sum(near_part[...], axis=0) + jnp.sum(far_part[...], axis=(0, 1))


def finish_kernel(every, near, order, meta, squares, recv, done, out, scale):
    comps, _, capacity, width = out.shape
    step = pl.program_id(0)

    @pl.when(step == 0)
    def _():
        total = jnp.sum(squares[...], keepdims=True)
        scale[...] = jnp.broadcast_to(1.0 / jnp.sqrt(total / every + 1e-06), scale.shape)

    @pl.when(step < near)
    def _():
        for c in range(comps):
            out[c, 0] = done[0, pl.ds(c, capacity, stride=comps), :] * scale[:1]

    @pl.when(step >= near)
    def _():
        lane = lax.broadcasted_iota(jnp.int32, (comps, width), 1)
        factor = scale[:comps]
        group = math.gcd(capacity, 64)
        first = step * capacity

        def some(t, _):
            start = first + t * group
            for k in range(group):
                mark = meta[start + k]
                fields = jnp.full((comps, width), mark, jnp.int32)
                ahead = lane + (lax.shift_right_logical(fields, 8) & 255)
                row = lax.shift_right_logical(mark, 16)
                head = recv[0, pl.ds(row, comps), :]
                tail = recv[0, pl.ds(row + comps, comps), :]
                joined = jnp.where(ahead >= width, head, tail)
                moved = pltpu.roll(joined, lax.shift_right_logical(mark, 8) & (width - 1), 1)
                value = jnp.where(lane < (fields & 255), moved * factor, 0.0)
                for c in range(comps):
                    out[c, 0, pl.ds(t * group + k, 1), :] = value[c : c + 1]
            return 0

        lax.fori_loop(0, capacity // group, some, 0)


def tier_sizes(capacity, n_y):
    def up(part):
        return -(-capacity * part // (64 * 8)) * 8

    direct = [(up(part), 0) for part in (52, 64)]
    if n_y % 2:
        return up(64), direct
    parts = ((38, 28), (39, 36), (40, 44), (44, 54))
    spilled = [(up(rows), up(extra)) for rows, extra in parts]
    return up(18), spilled + direct


def local(velocity, lengths, destinations):
    n_x, n_y, n_z = lax.axis_size("gx"), lax.axis_size("gy"), lax.axis_size("wa")
    comps, cells_x, cells_y, cells_z = velocity.shape
    width = BY * BZ
    nblk = cells_x * cells_y * cells_z // width
    writers = n_x * n_y
    capacity = max(2, 2 * nblk // writers)
    region = capacity + 8
    f32 = jnp.float32
    direct, tiers = tier_sizes(capacity, n_y)
    most_extra = max([8] + [extra for _, extra in tiers])
    senders = n_x * halves(n_y)
    beyond = max(1, writers - senders)

    smem = pl.BlockSpec(memory_space=pltpu.SMEM)
    vmem = pl.BlockSpec(memory_space=pltpu.VMEM)
    anywhere = pl.BlockSpec(memory_space=pl.ANY)
    dma = pltpu.SemaphoreType.DMA
    plan, tallies, y_faces, z_faces, need = pl.pallas_call(
        functools.partial(faces_kernel, writers, capacity, region, direct, n_y),
        out_shape=(
            jax.ShapeDtypeStruct((3, nblk // 128, 128), jnp.int32),
            jax.ShapeDtypeStruct((writers, 128), jnp.int32),
            jax.ShapeDtypeStruct((2, 2, cells_x, cells_z), f32),
            jax.ShapeDtypeStruct((2, 2, cells_y, cells_z), f32),
            jax.ShapeDtypeStruct((8, 128), f32),
        ),
        scratch_shapes=[pltpu.VMEM((writers, 128), f32)],
        name="faces",
    )(destinations.reshape(nblk // 128, 128), lengths.reshape(nblk // 128, 128), velocity)
    halos, tier = pl.pallas_call(
        functools.partial(halo_kernel, (n_x, n_y, n_z), tiers),
        out_shape=(
            jax.ShapeDtypeStruct((6, 2, max(cells_x, cells_y), cells_z), f32),
            jax.ShapeDtypeStruct((1,), jnp.int32),
        ),
        in_specs=[anywhere] * 3 + [vmem],
        out_specs=(anywhere, smem),
        scratch_shapes=[
            pltpu.VMEM((n_z,) + need.shape, f32),
            pltpu.VMEM((writers - 1, n_z) + need.shape, f32),
            dma((6,)),
            dma((6,)),
            dma((writers + n_z - 2,)),
            dma((writers + n_z - 2,)),
            dma,
        ],
        compiler_params=pltpu.CompilerParams(collective_id=1, has_side_effects=True),
        name="halo",
    )(velocity, y_faces, z_faces, need)

    table = jnp.asarray(split_table())
    outgoing, squares, meta, spill, starts = pl.pallas_call(
        functools.partial(blocks_kernel, n_x, n_y, region, direct),
        out_shape=(
            jax.ShapeDtypeStruct((writers * region * comps, width), f32),
            jax.ShapeDtypeStruct((8, cells_z), f32),
            jax.ShapeDtypeStruct((writers * capacity,), jnp.int32),
            jax.ShapeDtypeStruct((most_extra * comps // 8, 8, width), f32),
            jax.ShapeDtypeStruct((128,), jnp.int32),
        ),
        in_specs=[anywhere] * 3 + [vmem] * 3,
        out_specs=(vmem, vmem, smem, vmem, smem),
        scratch_shapes=[
            pltpu.VMEM((nblk * comps, width), f32),
            pltpu.SMEM((3 * nblk,), jnp.int32),
            pltpu.SMEM((writers, 128), jnp.int32),
            dma,
            dma,
            dma,
        ],
        compiler_params=pltpu.CompilerParams(vmem_limit_bytes=48 * 2**20),
        name="blocks",
    )(
        plan.reshape(3 * nblk),
        tallies,
        jnp.zeros((writers * capacity,), jnp.int32),
        velocity,
        halos,
        table,
    )
    outgoing = outgoing.reshape(writers, region * comps, width)
    part = min(capacity, 128)
    meta = meta.reshape(writers, capacity // part, part)

    def exchange(index, *operands):
        rows, extra = tiers[index]
        size = (rows - direct) * comps
        held = [pltpu.VMEM(((rows + 8) * comps, width), f32) for _ in range(senders)]
        relay = [
            pltpu.VMEM(((extra * comps + size) // 8, 8, width), f32),
            pltpu.VMEM((senders, size, width), f32),
            pltpu.VMEM((1, 128), jnp.int32),
            pltpu.SMEM((1, 128), jnp.int32),
            dma((senders,)),
            dma((senders,)),
            dma((2,)),
            dma((2,)),
            dma((2,)),
        ]
        return pl.pallas_call(
            functools.partial(exchange_kernel, n_x, n_y, n_z, comps, rows, direct, extra),
            out_shape=(
                jax.ShapeDtypeStruct((beyond, region * comps, width), f32),
                jax.ShapeDtypeStruct(squares.shape, f32),
                jax.ShapeDtypeStruct(meta.shape, jnp.int32),
                jax.ShapeDtypeStruct((senders, capacity * comps, width), f32),
            ),
            in_specs=[anywhere, vmem, anywhere, anywhere, anywhere],
            out_specs=(anywhere, vmem, anywhere, anywhere),
            scratch_shapes=[
                pltpu.VMEM((n_z,) + squares.shape, f32),
                pltpu.VMEM((writers - 1, n_z) + squares.shape, f32),
                pltpu.VMEM((senders, capacity * comps, width), f32),
                pltpu.SMEM((senders,) + meta.shape[1:], jnp.int32),
                dma((writers - 1,)),
                dma((writers - 1,)),
                dma((writers + n_z - 2,)),
                dma((writers + n_z - 2,)),
                dma((writers - 1,)),
                dma((writers - 1,)),
                dma((2,)),
                dma((senders,)),
                dma((senders,)),
            ]
            + held
            + (relay if extra else []),
            compiler_params=pltpu.CompilerParams(
                collective_id=2 + index, has_side_effects=True, vmem_limit_bytes=48 * 2**20
            ),
            name=f"exchange{rows}_{extra}",
        )(*operands)

    branches = [functools.partial(exchange, index) for index in range(len(tiers))]
    arrived, squares, heard, done = lax.switch(
        tier[0], branches, outgoing, squares, meta, spill, starts.reshape(1, 128)
    )

    near, far = plane_order(n_x, n_y, -1)
    order = jnp.stack([x * n_y + y for x, y, _ in near + far]).astype(jnp.int32)
    every = velocity.size * n_x * n_y * n_z
    received = pl.pallas_call(
        functools.partial(finish_kernel, float(every), senders),
        grid_spec=pltpu.PrefetchScalarGridSpec(
            num_scalar_prefetch=1,
            grid=(writers,),
            in_specs=[
                smem,
                pl.BlockSpec((8, cells_z), lambda s, order: (0, 0)),
                pl.BlockSpec(
                    (1, region * comps, width),
                    lambda s, order: (jnp.maximum(s - senders, 0), 0, 0),
                ),
                pl.BlockSpec(
                    (1, capacity * comps, width),
                    lambda s, order: (jnp.minimum(s, senders - 1), 0, 0),
                ),
            ],
            out_specs=pl.BlockSpec(
                (comps, 1, capacity, width), lambda s, order: (0, order[s], 0, 0)
            ),
            scratch_shapes=[pltpu.VMEM((8, width), f32)],
        ),
        out_shape=jax.ShapeDtypeStruct((comps, writers, capacity, width), f32),
        name="finish",
    )(order, heard.reshape(writers * capacity), squares, arrived, done)
    return received.reshape(1, 1, comps, writers, capacity, width)


def solution(mesh):
    return jax.shard_map(
        local,
        mesh=mesh,
        in_specs=(
            P(None, "gx", "gy", "wa"),
            P("gx", "gy", "wa", None),
            P("gx", "gy", "wa", None, None),
        ),
        out_specs=P(("gx", "gy"), "wa", None, None, None, None),
        check_vma=False,
    )
```

```python
import functools
import math

import jax
import jax.numpy as jnp
import numpy as np
from jax import lax
from jax.experimental import pallas as pl
from jax.experimental.pallas import tpu as pltpu
from jax.sharding import PartitionSpec as P

BY = 8
BZ = 16
UNROLL = 2
MESH = pl.DeviceIdType.MESH


def dct_table(count):
    freqs, points = np.arange(count)[:, None], np.arange(count)[None, :]
    table = np.cos(np.pi * (points + 0.5) * freqs / count) * np.sqrt(2.0 / count)
    return np.where(freqs == 0, table * np.sqrt(0.5), table)


def split_table():
    kron = np.kron(dct_table(BY), dct_table(BZ)).T.astype(np.float32)
    high = kron.astype(jnp.bfloat16)
    low = (kron - high.astype(np.float32)).astype(jnp.bfloat16)
    return np.block([[high, low], [high, np.zeros_like(low)]]).astype(jnp.bfloat16)


def spill_tiles(used, direct):
    return lax.shift_right_logical(jnp.maximum(used - direct, 0) + 7, 3)


def plan_blocks(writers, capacity, region, direct, n_y, comps, t, kept, plan, counts, need, sums):
    rows, lanes = t.shape
    shape = (lanes, lanes)
    upper = (
        lax.broadcasted_iota(jnp.int32, shape, 0) < lax.broadcasted_iota(jnp.int32, shape, 1)
    ).astype(jnp.float32).astype(jnp.bfloat16)
    square = (rows, rows)
    lower = (
        lax.broadcasted_iota(jnp.int32, square, 1) < lax.broadcasted_iota(jnp.int32, square, 0)
    ).astype(jnp.float32).astype(jnp.bfloat16)
    weight = kept.astype(jnp.float32)

    def body(w, acc):
        spot, start, site = acc
        mine = t == w
        ones = mine.astype(jnp.float32)
        sizes = jnp.where(mine, weight, 0.0)
        both = jnp.concatenate([ones, sizes], axis=0).astype(jnp.bfloat16)
        sums[pl.ds(w, 1), :] = jnp.sum(sizes, axis=0, keepdims=True)
        inner = jnp.dot(both, upper, preferred_element_type=jnp.float32)
        side = jnp.concatenate([ones, sizes], axis=1).astype(jnp.bfloat16)
        before = jnp.dot(lower, side, preferred_element_type=jnp.float32)
        rank = inner[:rows] + jnp.sum(before[:, :lanes], axis=1, keepdims=True)
        offset = inner[rows:] + jnp.sum(before[:, lanes:], axis=1, keepdims=True)
        spot = jnp.where(mine, w * capacity + rank.astype(jnp.int32), spot)
        offset = offset.astype(jnp.int32)
        start = jnp.where(mine, offset, start)
        site = jnp.where(mine, w * region, site)
        return spot, start, site

    none = jnp.zeros_like(t)
    spot, start, site = lax.fori_loop(0, writers, body, (none, none, none), unroll=8)
    used = jnp.sum(sums[...], axis=1, keepdims=True).astype(jnp.int32)
    used = jnp.broadcast_to(lax.shift_right_logical(used + (lanes - 1), 7), counts.shape)
    counts[...] = used
    writer = lax.broadcasted_iota(jnp.int32, counts.shape, 0)
    half = max(1, n_y // 2)
    far_side = lax.div(lax.rem(writer, n_y), half) != lax.div(lax.axis_index("gy"), half)
    over = jnp.where(far_side, spill_tiles(used, direct) * 8, 0)
    most = jnp.max(used.astype(jnp.float32), axis=0, keepdims=True)
    extra = jnp.sum(over.astype(jnp.float32), axis=0, keepdims=True)
    line = lax.broadcasted_iota(jnp.int32, need.shape, 0)
    need[...] = jnp.where(line == 0, most, jnp.where(line == 1, extra, 0.0))
    shift = start & (lanes - 1)
    row = lax.shift_right_logical(start, lanes.bit_length() - 1)
    plan[2] = spot
    plan[0] = (row + site) * (comps << 16) + shift
    plan[1] = row * (comps << 16) + (lanes - shift) * 256 + kept


def plane_offsets(n_x, n_y):
    offsets = [(i, j) for i in range(n_x) for j in range(n_y) if i or j]
    return sorted(offsets, key=lambda o: (bool(o[0]) and bool(o[1]), min(o[1], n_y - o[1])))


def plane_peers(n_x, n_y):
    a, b, c = (lax.axis_index(axis) for axis in ("gx", "gy", "wa"))
    return [(lax.rem(a + i, n_x), lax.rem(b + j, n_y), c) for i, j in plane_offsets(n_x, n_y)]


def line_mates(n_z):
    a, b, c = (lax.axis_index(axis) for axis in ("gx", "gy", "wa"))
    return [(a, b, lax.rem(c + k, n_z)) for k in range(1, n_z)]


def send_to(src, dst, send_sem, recv_sem, device):
    copy = pltpu.make_async_remote_copy(
        src_ref=src,
        dst_ref=dst,
        send_sem=send_sem,
        recv_sem=recv_sem,
        device_id=device,
        device_id_type=MESH,
    )
    copy.start()
    return copy


def spill_tiles(used, direct):
    return lax.shift_right_logical(jnp.maximum(used - direct, 0) + 7, 3)


def front_kernel(
    sizes, tiers, capacity, region, direct, targets, lens, vel, plan, counts, halos, tier, order,
    z_faces, need, sums, near_part, far_part, send_sem, recv_sem, part_send, part_recv, own_sem,
):
    place = [lax.axis_index(axis) for axis in ("gx", "gy", "wa")]
    n_x, n_y, n_z = sizes
    comps, cells_x, cells_y, cells_z = vel.shape
    writers = n_x * n_y

    def beside(axis, step):
        size = sizes[axis]
        moved = lax.rem(place[axis] + step + size, size)
        return tuple(moved if i == axis else p for i, p in enumerate(place))

    across, along = pl.ds(0, cells_y), pl.ds(0, cells_x)
    peers, mates = plane_peers(n_x, n_y), line_mates(n_z)
    others = [beside(axis, step) for axis in range(3) for step in (1, -1)] + peers + mates
    barrier = pltpu.get_barrier_semaphore()
    for device in others:
        pl.semaphore_signal(barrier, inc=1, device_id=device, device_id_type=MESH)
    plan_blocks(
        writers, capacity, region, direct, n_y, comps, targets[...], lens[...], plan, counts, need,
        sums,
    )
    pl.semaphore_wait(barrier, len(others))
    moves = [
        (vel.at[pl.ds(1, 2), cells_x - 1], halos.at[0, :, across], beside(0, 1)),
        (vel.at[pl.ds(1, 2), 0], halos.at[1, :, across], beside(0, -1)),
    ]
    for i, comp in enumerate((0, 2)):
        moves += [
            (vel.at[comp, :, cells_y - 1], halos.at[2, i, along], beside(1, 1)),
            (vel.at[comp, :, 0], halos.at[3, i, along], beside(1, -1)),
        ]
    copies = [
        send_to(src, dst, send_sem.at[k], recv_sem.at[k], device)
        for k, (src, dst, device) in enumerate(moves)
    ]
    c = place[2]
    own = pltpu.make_async_copy(need, near_part.at[c], own_sem)
    own.start()
    first = [
        send_to(need, near_part.at[c], part_send.at[k], part_recv.at[k], device)
        for k, device in enumerate(mates)
    ]
    lane = lax.broadcasted_iota(jnp.int32, (cells_y, cells_z), 1)

    def plane(x, acc):
        here = lane == x
        rolled = [
            pltpu.roll(vel[comp, x], lax.rem(x + last, cells_z), 1)
            for last in range(2)
            for comp in (0, 1)
        ]
        return tuple(jnp.where(here, new, old) for new, old in zip(rolled, acc))

    zero = jnp.zeros((cells_y, cells_z), jnp.float32)
    columns = lax.fori_loop(0, cells_x, plane, (zero,) * 4, unroll=4)
    for last in range(2):
        for i in range(2):
            z_faces[last, i] = columns[2 * last + i]
    near, far = plane_order(n_x, n_y, -1)
    for k, (x, y, _) in enumerate(near + far):
        order[k] = x * n_y + y
    own.wait()
    for copy in first:
        copy.wait()
    for k, device in enumerate(peers):
        sem = n_z - 1 + k
        copies.append(
            send_to(near_part, far_part.at[k], part_send.at[sem], part_recv.at[sem], device)
        )
    k = len(moves)
    for src, spot, step in ((1, 4, 1), (0, 5, -1)):
        copies.append(
            send_to(
                z_faces.at[src], halos.at[spot, :, across], send_sem.at[k], recv_sem.at[k],
                beside(2, step),
            )
        )
        k += 1
    for copy in copies:
        copy.wait()
    most = jnp.maximum(jnp.max(near_part[...], axis=0), jnp.max(far_part[...], axis=(0, 1)))
    pair, extra = jnp.max(most[0:1]), jnp.max(most[1:2])
    chosen = jnp.int32(len(tiers) - 1)
    for index in reversed(range(len(tiers) - 1)):
        rows, spill = tiers[index]
        fits = pair <= rows
        if spill:
            fits = jnp.logical_and(fits, extra <= spill)
        chosen = jnp.where(fits, index, chosen)
    tier[0] = chosen


def block_rows(plane):
    cells_y, cells_z = plane.shape
    tiles = plane.reshape(cells_y // BY, BY, cells_z)
    sub = lax.broadcasted_iota(jnp.int32, tiles.shape, 1)
    group = lax.broadcasted_iota(jnp.int32, tiles.shape, 2) // BZ
    k = 1
    while k < BY:
        s_bit, g_bit = (sub & k) != 0, (group & k) != 0
        fwd = pltpu.roll(pltpu.roll(tiles, BY - k, 1), k * BZ, 2)
        back = pltpu.roll(pltpu.roll(tiles, k, 1), cells_z - k * BZ, 2)
        tiles = jnp.where(s_bit == g_bit, tiles, jnp.where(g_bit, fwd, back))
        k *= 2
    return tiles.reshape(cells_y, cells_z)


def blocks_kernel(
    n_x, n_y, region, direct, lists, tallies, blank, vel, halos, table, out, squares, meta, spill,
    starts, coeffs, plan, counts, meta_sem, plan_sem, count_sem,
):
    comps, cells_x, cells_y, cells_z = vel.shape
    nblk = coeffs.shape[0] // comps
    per_plane = nblk // cells_x
    width = out.shape[1]
    row = lax.broadcasted_iota(jnp.int32, (cells_y, cells_z), 0)
    lane = lax.broadcasted_iota(jnp.int32, (cells_y, cells_z), 1)
    clear = pltpu.make_async_copy(blank, meta, meta_sem)
    clear.start()
    fetch = pltpu.make_async_copy(lists, plan, plan_sem)
    fetch.start()
    tally = pltpu.make_async_copy(tallies, counts, count_sem)
    tally.start()

    def plane(x, acc):
        u, v, w = vel[0, x], vel[1, x], vel[2, x]

        def along_x(comp):
            nxt = jnp.where(
                x == cells_x - 1, halos[1, comp - 1, :cells_y], vel[comp, jnp.minimum(x + 1, cells_x - 1)]
            )
            prv = jnp.where(x == 0, halos[0, comp - 1, :cells_y], vel[comp, jnp.maximum(x - 1, 0)])
            return (nxt - prv) * 0.5

        def along_y(f, face):
            nxt = jnp.where(
                row == cells_y - 1, halos[3, face, pl.ds(x, 1), :], pltpu.roll(f, cells_y - 1, 0)
            )
            prv = jnp.where(row == 0, halos[2, face, pl.ds(x, 1), :], pltpu.roll(f, 1, 0))
            return (nxt - prv) * 0.5

        def along_z(f, face):
            after = pltpu.roll(halos[5, face, :cells_y], cells_z - 1 - x, 1)
            before = pltpu.roll(halos[4, face, :cells_y], lax.rem(cells_z - x, cells_z), 1)
            nxt = jnp.where(lane == cells_z - 1, after, pltpu.roll(f, cells_z - 1, 1))
            prv = jnp.where(lane == 0, before, pltpu.roll(f, 1, 1))
            return (nxt - prv) * 0.5

        curl = (
            along_y(w, 1) - along_z(v, 1),
            along_z(u, 0) - along_x(2),
            along_x(1) - along_y(u, 0),
        )
        for c in curl:
            acc = acc + jnp.sum((c * c).reshape(cells_y // 8, 8, cells_z), axis=0)
        flat = jnp.concatenate([block_rows(c) for c in curl], axis=0)
        high = flat.astype(jnp.bfloat16)
        low = (flat - high.astype(jnp.float32)).astype(jnp.bfloat16)
        both = jnp.dot(
            jnp.concatenate([high, low], axis=1), table[...], preferred_element_type=jnp.float32
        )
        result = both[:, :width] + both[:, width:]
        start = x * (comps * per_plane)
        for c in range(comps):
            coeffs[pl.ds(start + c, per_plane, stride=comps), :] = result[
                c * per_plane : (c + 1) * per_plane
            ]
        return acc

    spread = lax.broadcasted_iota(jnp.int32, (comps, width), 1)
    group = 8

    def place(x):
        for start in range(0, per_plane, group):
            found = []
            for k in range(start, min(start + group, per_plane)):
                i = x * per_plane + k
                word = plan[i]
                meta[plan[2 * nblk + i]] = plan[nblk + i]
                shift = word & (width - 1)
                row = lax.shift_right_logical(word, 16)
                moved = pltpu.roll(coeffs[pl.ds(i * comps, comps), :], shift, 1)
                found.append((row, moved, spread >= shift))
            for row, moved, mask in found:
                pltpu.store(out.at[pl.ds(row, comps), :], moved, mask=mask)
                out[pl.ds(row + comps, comps), :] = moved

    together = next(n for n in (UNROLL, 2, 1) if cells_x % n == 0)

    def step(t, acc):
        for k in range(together):
            place((t - 1) * together + k)
        return planes(t, acc)

    def planes(t, acc):
        for k in range(together):
            acc = plane(t * together + k, acc)
        return acc

    clear.wait()
    fetch.wait()
    tally.wait()
    first = planes(0, jnp.zeros((8, cells_z), jnp.float32))
    squares[...] = lax.fori_loop(1, cells_x // together, step, first)
    for k in range(together):
        place(cells_x - together + k)

    half = max(1, n_y // 2)
    facing = lax.rem(lax.div(lax.axis_index("gy"), half) + 1, 2) * half
    most = spill.shape[0] // comps

    def segment(j, begin):
        writer = lax.div(j, half) * n_y + facing + lax.rem(j, half)
        tiles = jnp.minimum(spill_tiles(counts[writer, 0], direct), most - begin)
        starts[j] = begin
        source = (writer * region + direct) * comps

        def tile(i, _):
            for c in range(comps):
                at = source + (i * comps + c) * 8
                spill[(begin + i) * comps + c] = out[pl.ds(pl.multiple_of(at, 8), 8), :]
            return 0

        lax.fori_loop(0, tiles, tile, 0)
        return begin + tiles

    lax.fori_loop(0, n_x * half, segment, jnp.int32(0))


def halves(n_y):
    return n_y if n_y % 2 else n_y // 2


def plane_order(n_x, n_y, sign):
    a, b, c = (lax.axis_index(axis) for axis in ("gx", "gy", "wa"))
    half = halves(n_y)
    mine = lax.rem(b, half)
    base = b - mine
    steps = [(i, j) for i in range(n_x) for j in range(half)]

    def at(base, i, j):
        x = lax.rem(a + sign * i + n_x, n_x)
        return (x, base + lax.rem(mine + sign * j + half, half), c)

    near = [at(base, i, j) for i, j in steps]
    other = lax.rem(base + half, n_y)
    far = [at(other, i, j) for i, j in steps] if half < n_y else []
    return near, far


def unpack(count, marks, source, target, lane, at):
    comps, width = lane.shape
    group = math.gcd(marks[0].shape[-1], 32 if count <= 4 else 8)
    lists, k = marks
    per_line = lists.shape[2] // group

    def some(t, _):
        line = lax.div(t, per_line)
        start = lax.rem(t, per_line) * group
        for i in range(group):
            mark = lists[k, line, start + i]
            fields = jnp.full((comps, width), mark, jnp.int32)
            ahead = lane + (lax.shift_right_logical(fields, 8) & 255)
            row = lax.shift_right_logical(mark, 16)
            head = source[pl.ds(row, comps), :]
            tail = source[pl.ds(row + comps, comps), :]
            joined = jnp.where(ahead >= width, head, tail)
            moved = pltpu.roll(joined, lax.shift_right_logical(mark, 8) & (width - 1), 1)
            value = jnp.where(lane < (fields & 255), moved, 0.0)
            target[at, pl.ds((t * group + i) * comps, comps), :] = value
        return 0

    lax.fori_loop(0, lists.shape[1] * per_line, some, 0)


def exchange_kernel(
    n_x, n_y, n_z, comps, rows, direct, extra, send, squares, meta, spill, starts, recv, total, heard,
    done, near_part, far_part, stage, marks, send_sem, recv_sem, part_send, part_recv, word_send,
    word_recv, own_sem, done_sem, mark_sem, *rest,
):
    c = lax.axis_index("wa")
    near, far = plane_order(n_x, n_y, 1)
    me = near[0][0] * n_y + near[0][1]
    held, relay = rest[: len(near)], rest[len(near) :]
    peers, mates = near[1:] + far, line_mates(n_z)
    barrier = pltpu.get_barrier_semaphore()
    for device in mates + peers:
        pl.semaphore_signal(barrier, inc=1, device_id=device, device_id_type=MESH)
    pl.semaphore_wait(barrier, len(peers) + len(mates))

    def number(device):
        return device[0] * n_y + device[1]

    whole = pl.ds(0, rows * comps)
    own = [
        pltpu.make_async_copy(squares, near_part.at[c], own_sem.at[0]),
        pltpu.make_async_copy(meta.at[me], marks.at[0], mark_sem.at[0]),
        pltpu.make_async_copy(send.at[me, whole], held[0].at[whole], own_sem.at[1]),
    ]
    for copy in own:
        copy.start()
    first = [
        send_to(squares, near_part.at[c], part_send.at[k], part_recv.at[k], device)
        for k, device in enumerate(mates)
    ]
    relays, copies, words, blocks = [], [], [], []
    if extra:
        (
            landed, ready, begins, places, relay_send, relay_recv, spill_send, spill_recv, begin_sem
        ) = relay
        tiles = pl.ds(0, extra * comps // 8)
        relays = [
            send_to(starts, begins, spill_send.at[0], spill_recv.at[0], far[0]),
            send_to(spill.at[tiles], landed.at[tiles], spill_send.at[1], spill_recv.at[1], far[0]),
        ]
    for k, device in enumerate(peers):
        words.append(
            send_to(meta.at[number(device)], heard.at[k + 1], word_send.at[k], word_recv.at[k], device)
        )
    short = pl.ds(0, direct * comps) if extra else whole
    for k, device in enumerate(peers):
        if k + 1 < len(near):
            used, target = whole, held[k + 1].at[whole]
        else:
            used, target = short, recv.at[k + 1 - len(near), short]
        blocks.append(
            send_to(send.at[number(device), used], target, send_sem.at[k], recv_sem.at[k], device)
        )
    own[0].wait()
    for copy in first:
        copy.wait()
    for k, device in enumerate(peers):
        sem = n_z - 1 + k
        copies.append(
            send_to(near_part, far_part.at[k], part_send.at[sem], part_recv.at[sem], device)
        )
    if extra:
        relays[0].wait()
        load = pltpu.make_async_copy(begins, places, begin_sem.at[0])
        load.start()
        load.wait()
        relays[1].wait()
        size = (rows - direct) * comps
        half = halves(n_y)
        for k, (x, y, _) in enumerate(near):
            begin = places[0, x * half + lax.rem(y, half)] * comps

            def tile(i, _, k=k, begin=begin):
                ready[k, pl.ds(pl.multiple_of(i * 8, 8), 8), :] = landed[begin + i]
                return 0

            lax.fori_loop(0, size // 8, tile, 0)
        past = pl.ds(direct * comps, size)
        for k, device in enumerate(near):
            if k:
                copies.append(
                    send_to(
                        ready.at[k], recv.at[k, past], relay_send.at[k], relay_recv.at[k], device
                    )
                )
        keep = pltpu.make_async_copy(ready.at[0], recv.at[0, past], begin_sem.at[1])
        keep.start()
        keep.wait()
    lane = lax.broadcasted_iota(jnp.int32, (comps, send.shape[2]), 1)
    outs = []
    for k in range(len(near)):
        if k:
            words[k - 1].wait()
            load = pltpu.make_async_copy(heard.at[k], marks.at[k], mark_sem.at[k])
            load.start()
            load.wait()
            blocks[k - 1].wait()
        else:
            own[1].wait()
            own[2].wait()
        unpack(len(near), (marks, k), held[k], stage, lane, k)
        out = pltpu.make_async_copy(stage.at[k], done.at[k], done_sem.at[k])
        out.start()
        outs.append(out)
    for copy in words[len(near) - 1 :] + blocks[len(near) - 1 :] + copies + outs:
        copy.wait()
    total[...] = jnp.sum(near_part[...], axis=0) + jnp.sum(far_part[...], axis=(0, 1))


def finish_kernel(every, near, order, meta, squares, recv, done, out, scale):
    comps, _, capacity, width = out.shape
    step = pl.program_id(0)

    @pl.when(step == 0)
    def _():
        total = jnp.sum(squares[...], keepdims=True)
        scale[...] = jnp.broadcast_to(1.0 / jnp.sqrt(total / every + 1e-06), scale.shape)

    @pl.when(step < near)
    def _():
        for c in range(comps):
            out[c, 0] = done[0, pl.ds(c, capacity, stride=comps), :] * scale[:1]

    @pl.when(step >= near)
    def _():
        lane = lax.broadcasted_iota(jnp.int32, (comps, width), 1)
        factor = scale[:comps]
        group = math.gcd(capacity, 64)
        first = step * capacity

        def some(t, _):
            start = first + t * group
            for k in range(group):
                mark = meta[start + k]
                fields = jnp.full((comps, width), mark, jnp.int32)
                ahead = lane + (lax.shift_right_logical(fields, 8) & 255)
                row = lax.shift_right_logical(mark, 16)
                head = recv[0, pl.ds(row, comps), :]
                tail = recv[0, pl.ds(row + comps, comps), :]
                joined = jnp.where(ahead >= width, head, tail)
                moved = pltpu.roll(joined, lax.shift_right_logical(mark, 8) & (width - 1), 1)
                value = jnp.where(lane < (fields & 255), moved * factor, 0.0)
                for c in range(comps):
                    out[c, 0, pl.ds(t * group + k, 1), :] = value[c : c + 1]
            return 0

        lax.fori_loop(0, capacity // group, some, 0)


def tier_sizes(capacity, n_y):
    def up(part):
        return -(-capacity * part // (64 * 8)) * 8

    direct = [(up(part), 0) for part in (52, 64)]
    if n_y % 2:
        return up(64), direct
    parts = ((38, 28), (39, 36), (39, 44), (40, 54))
    spilled = [(up(rows), up(extra)) for rows, extra in parts]
    return up(18), spilled + direct


def local(velocity, lengths, destinations):
    n_x, n_y, n_z = lax.axis_size("gx"), lax.axis_size("gy"), lax.axis_size("wa")
    comps, cells_x, cells_y, cells_z = velocity.shape
    width = BY * BZ
    nblk = cells_x * cells_y * cells_z // width
    writers = n_x * n_y
    capacity = max(2, 2 * nblk // writers)
    region = capacity + 8
    f32 = jnp.float32
    direct, tiers = tier_sizes(capacity, n_y)
    most_extra = max([8] + [extra for _, extra in tiers])
    senders = n_x * halves(n_y)
    beyond = max(1, writers - senders)

    smem = pl.BlockSpec(memory_space=pltpu.SMEM)
    vmem = pl.BlockSpec(memory_space=pltpu.VMEM)
    anywhere = pl.BlockSpec(memory_space=pl.ANY)
    dma = pltpu.SemaphoreType.DMA
    plan, tallies, halos, tier, order = pl.pallas_call(
        functools.partial(front_kernel, (n_x, n_y, n_z), tiers, capacity, region, direct),
        out_shape=(
            jax.ShapeDtypeStruct((3, nblk // 128, 128), jnp.int32),
            jax.ShapeDtypeStruct((writers, 128), jnp.int32),
            jax.ShapeDtypeStruct((6, 2, max(cells_x, cells_y), cells_z), f32),
            jax.ShapeDtypeStruct((1,), jnp.int32),
            jax.ShapeDtypeStruct((writers,), jnp.int32),
        ),
        in_specs=[vmem, vmem, vmem],
        out_specs=(vmem, vmem, vmem, smem, smem),
        scratch_shapes=[
            pltpu.VMEM((2, 2, cells_y, cells_z), f32),
            pltpu.VMEM((8, 128), f32),
            pltpu.VMEM((writers, 128), f32),
            pltpu.VMEM((n_z, 8, 128), f32),
            pltpu.VMEM((writers - 1, n_z, 8, 128), f32),
            dma((8,)),
            dma((8,)),
            dma((writers + n_z - 2,)),
            dma((writers + n_z - 2,)),
            dma,
        ],
        compiler_params=pltpu.CompilerParams(
            collective_id=1, has_side_effects=True, vmem_limit_bytes=16 * 2**20
        ),
        name="front",
    )(destinations.reshape(nblk // 128, 128), lengths.reshape(nblk // 128, 128), velocity)

    table = jnp.asarray(split_table())
    outgoing, squares, meta, spill, starts = pl.pallas_call(
        functools.partial(blocks_kernel, n_x, n_y, region, direct),
        out_shape=(
            jax.ShapeDtypeStruct((writers * region * comps, width), f32),
            jax.ShapeDtypeStruct((8, cells_z), f32),
            jax.ShapeDtypeStruct((writers * capacity,), jnp.int32),
            jax.ShapeDtypeStruct((most_extra * comps // 8, 8, width), f32),
            jax.ShapeDtypeStruct((128,), jnp.int32),
        ),
        in_specs=[anywhere] * 3 + [vmem] * 3,
        out_specs=(vmem, vmem, smem, vmem, smem),
        scratch_shapes=[
            pltpu.VMEM((nblk * comps, width), f32),
            pltpu.SMEM((3 * nblk,), jnp.int32),
            pltpu.SMEM((writers, 128), jnp.int32),
            dma,
            dma,
            dma,
        ],
        compiler_params=pltpu.CompilerParams(vmem_limit_bytes=48 * 2**20),
        name="blocks",
    )(
        plan.reshape(3 * nblk),
        tallies,
        jnp.zeros((writers * capacity,), jnp.int32),
        velocity,
        halos,
        table,
    )
    outgoing = outgoing.reshape(writers, region * comps, width)
    part = min(capacity, 128)
    meta = meta.reshape(writers, capacity // part, part)

    def exchange(index, *operands):
        rows, extra = tiers[index]
        size = (rows - direct) * comps
        held = [pltpu.VMEM(((rows + 8) * comps, width), f32) for _ in range(senders)]
        relay = [
            pltpu.VMEM(((extra * comps + size) // 8, 8, width), f32),
            pltpu.VMEM((senders, size, width), f32),
            pltpu.VMEM((1, 128), jnp.int32),
            pltpu.SMEM((1, 128), jnp.int32),
            dma((senders,)),
            dma((senders,)),
            dma((2,)),
            dma((2,)),
            dma((2,)),
        ]
        return pl.pallas_call(
            functools.partial(exchange_kernel, n_x, n_y, n_z, comps, rows, direct, extra),
            out_shape=(
                jax.ShapeDtypeStruct((beyond, region * comps, width), f32),
                jax.ShapeDtypeStruct(squares.shape, f32),
                jax.ShapeDtypeStruct(meta.shape, jnp.int32),
                jax.ShapeDtypeStruct((senders, capacity * comps, width), f32),
            ),
            in_specs=[anywhere, vmem, anywhere, anywhere, anywhere],
            out_specs=(anywhere, vmem, anywhere, anywhere),
            scratch_shapes=[
                pltpu.VMEM((n_z,) + squares.shape, f32),
                pltpu.VMEM((writers - 1, n_z) + squares.shape, f32),
                pltpu.VMEM((senders, capacity * comps, width), f32),
                pltpu.SMEM((senders,) + meta.shape[1:], jnp.int32),
                dma((writers - 1,)),
                dma((writers - 1,)),
                dma((writers + n_z - 2,)),
                dma((writers + n_z - 2,)),
                dma((writers - 1,)),
                dma((writers - 1,)),
                dma((2,)),
                dma((senders,)),
                dma((senders,)),
            ]
            + held
            + (relay if extra else []),
            compiler_params=pltpu.CompilerParams(
                collective_id=2 + index, has_side_effects=True, vmem_limit_bytes=48 * 2**20
            ),
            name=f"exchange{rows}_{extra}",
        )(*operands)

    branches = [functools.partial(exchange, index) for index in range(len(tiers))]
    arrived, squares, heard, done = lax.switch(
        tier[0], branches, outgoing, squares, meta, spill, starts.reshape(1, 128)
    )

    every = velocity.size * n_x * n_y * n_z
    received = pl.pallas_call(
        functools.partial(finish_kernel, float(every), senders),
        grid_spec=pltpu.PrefetchScalarGridSpec(
            num_scalar_prefetch=1,
            grid=(writers,),
            in_specs=[
                smem,
                pl.BlockSpec((8, cells_z), lambda s, order: (0, 0)),
                pl.BlockSpec(
                    (1, region * comps, width),
                    lambda s, order: (jnp.maximum(s - senders, 0), 0, 0),
                ),
                pl.BlockSpec(
                    (1, capacity * comps, width),
                    lambda s, order: (jnp.minimum(s, senders - 1), 0, 0),
                ),
            ],
            out_specs=pl.BlockSpec(
                (comps, 1, capacity, width), lambda s, order: (0, order[s], 0, 0)
            ),
            scratch_shapes=[pltpu.VMEM((8, width), f32)],
        ),
        out_shape=jax.ShapeDtypeStruct((comps, writers, capacity, width), f32),
        name="finish",
    )(order, heard.reshape(writers * capacity), squares, arrived, done)
    return received.reshape(1, 1, comps, writers, capacity, width)


def solution(mesh):
    return jax.shard_map(
        local,
        mesh=mesh,
        in_specs=(
            P(None, "gx", "gy", "wa"),
            P("gx", "gy", "wa", None),
            P("gx", "gy", "wa", None, None),
        ),
        out_specs=P(("gx", "gy"), "wa", None, None, None, None),
        check_vma=False,
    )
```

```python
import functools
import math

import jax
import jax.numpy as jnp
import numpy as np
from jax import lax
from jax.experimental import pallas as pl
from jax.experimental.pallas import tpu as pltpu
from jax.sharding import PartitionSpec as P

BY = 8
BZ = 16
UNROLL = 2
MESH = pl.DeviceIdType.MESH


def dct_table(count):
    freqs, points = np.arange(count)[:, None], np.arange(count)[None, :]
    table = np.cos(np.pi * (points + 0.5) * freqs / count) * np.sqrt(2.0 / count)
    return np.where(freqs == 0, table * np.sqrt(0.5), table)


def split_table():
    kron = np.kron(dct_table(BY), dct_table(BZ)).T.astype(np.float32)
    high = kron.astype(jnp.bfloat16)
    low = (kron - high.astype(np.float32)).astype(jnp.bfloat16)
    return np.block([[high, low], [high, np.zeros_like(low)]]).astype(jnp.bfloat16)


def spill_tiles(used, direct):
    return lax.shift_right_logical(jnp.maximum(used - direct, 0) + 7, 3)


def plan_blocks(writers, capacity, region, direct, n_y, comps, t, kept, plan, counts, need, sums):
    rows, lanes = t.shape
    shape = (lanes, lanes)
    upper = (
        lax.broadcasted_iota(jnp.int32, shape, 0) < lax.broadcasted_iota(jnp.int32, shape, 1)
    ).astype(jnp.float32).astype(jnp.bfloat16)
    square = (rows, rows)
    lower = (
        lax.broadcasted_iota(jnp.int32, square, 1) < lax.broadcasted_iota(jnp.int32, square, 0)
    ).astype(jnp.float32).astype(jnp.bfloat16)
    weight = kept.astype(jnp.float32)

    def body(w, acc):
        spot, start, site = acc
        mine = t == w
        ones = mine.astype(jnp.float32)
        sizes = jnp.where(mine, weight, 0.0)
        both = jnp.concatenate([ones, sizes], axis=0).astype(jnp.bfloat16)
        sums[pl.ds(w, 1), :] = jnp.sum(sizes, axis=0, keepdims=True)
        inner = jnp.dot(both, upper, preferred_element_type=jnp.float32)
        side = jnp.concatenate([ones, sizes], axis=1).astype(jnp.bfloat16)
        before = jnp.dot(lower, side, preferred_element_type=jnp.float32)
        rank = inner[:rows] + jnp.sum(before[:, :lanes], axis=1, keepdims=True)
        offset = inner[rows:] + jnp.sum(before[:, lanes:], axis=1, keepdims=True)
        spot = jnp.where(mine, w * capacity + rank.astype(jnp.int32), spot)
        offset = offset.astype(jnp.int32)
        start = jnp.where(mine, offset, start)
        site = jnp.where(mine, w * region, site)
        return spot, start, site

    none = jnp.zeros_like(t)
    spot, start, site = lax.fori_loop(0, writers, body, (none, none, none), unroll=8)
    used = jnp.sum(sums[...], axis=1, keepdims=True).astype(jnp.int32)
    used = jnp.broadcast_to(lax.shift_right_logical(used + (lanes - 1), 7), counts.shape)
    counts[...] = used
    writer = lax.broadcasted_iota(jnp.int32, counts.shape, 0)
    half = max(1, n_y // 2)
    far_side = lax.div(lax.rem(writer, n_y), half) != lax.div(lax.axis_index("gy"), half)
    over = jnp.where(far_side, spill_tiles(used, direct) * 8, 0)
    most = jnp.max(used.astype(jnp.float32), axis=0, keepdims=True)
    extra = jnp.sum(over.astype(jnp.float32), axis=0, keepdims=True)
    line = lax.broadcasted_iota(jnp.int32, need.shape, 0)
    need[...] = jnp.where(line == 0, most, jnp.where(line == 1, extra, 0.0))
    shift = start & (lanes - 1)
    row = lax.shift_right_logical(start, lanes.bit_length() - 1)
    plan[2] = spot
    plan[0] = (row + site) * (comps << 16) + shift
    plan[1] = row * (comps << 16) + (lanes - shift) * 256 + kept


def plane_offsets(n_x, n_y):
    offsets = [(i, j) for i in range(n_x) for j in range(n_y) if i or j]
    return sorted(offsets, key=lambda o: (bool(o[0]) and bool(o[1]), min(o[1], n_y - o[1])))


def plane_peers(n_x, n_y):
    a, b, c = (lax.axis_index(axis) for axis in ("gx", "gy", "wa"))
    return [(lax.rem(a + i, n_x), lax.rem(b + j, n_y), c) for i, j in plane_offsets(n_x, n_y)]


def line_mates(n_z):
    a, b, c = (lax.axis_index(axis) for axis in ("gx", "gy", "wa"))
    return [(a, b, lax.rem(c + k, n_z)) for k in range(1, n_z)]


def send_to(src, dst, send_sem, recv_sem, device):
    copy = pltpu.make_async_remote_copy(
        src_ref=src,
        dst_ref=dst,
        send_sem=send_sem,
        recv_sem=recv_sem,
        device_id=device,
        device_id_type=MESH,
    )
    copy.start()
    return copy


def spill_tiles(used, direct):
    return lax.shift_right_logical(jnp.maximum(used - direct, 0) + 7, 3)


def front_kernel(
    sizes, tiers, capacity, region, direct, targets, lens, vel, plan, counts, inside, halos, tier, order,
    z_faces, need, sums, near_part, far_part, send_sem, recv_sem, part_send, part_recv, own_sem,
):
    place = [lax.axis_index(axis) for axis in ("gx", "gy", "wa")]
    n_x, n_y, n_z = sizes
    comps, cells_x, cells_y, cells_z = vel.shape
    writers = n_x * n_y
    load = pltpu.make_async_copy(vel, inside, own_sem.at[0])
    load.start()

    def beside(axis, step):
        size = sizes[axis]
        moved = lax.rem(place[axis] + step + size, size)
        return tuple(moved if i == axis else p for i, p in enumerate(place))

    across, along = pl.ds(0, cells_y), pl.ds(0, cells_x)
    peers, mates = plane_peers(n_x, n_y), line_mates(n_z)
    others = [beside(axis, step) for axis in range(3) for step in (1, -1)] + peers + mates
    barrier = pltpu.get_barrier_semaphore()
    for device in others:
        pl.semaphore_signal(barrier, inc=1, device_id=device, device_id_type=MESH)
    plan_blocks(
        writers, capacity, region, direct, n_y, comps, targets[...], lens[...], plan, counts, need,
        sums,
    )
    pl.semaphore_wait(barrier, len(others))
    moves = [
        (vel.at[pl.ds(1, 2), cells_x - 1], halos.at[0, :, across], beside(0, 1)),
        (vel.at[pl.ds(1, 2), 0], halos.at[1, :, across], beside(0, -1)),
    ]
    for i, comp in enumerate((0, 2)):
        moves += [
            (vel.at[comp, :, cells_y - 1], halos.at[2, i, along], beside(1, 1)),
            (vel.at[comp, :, 0], halos.at[3, i, along], beside(1, -1)),
        ]
    copies = [
        send_to(src, dst, send_sem.at[k], recv_sem.at[k], device)
        for k, (src, dst, device) in enumerate(moves)
    ]
    c = place[2]
    own = pltpu.make_async_copy(need, near_part.at[c], own_sem.at[1])
    own.start()
    first = [
        send_to(need, near_part.at[c], part_send.at[k], part_recv.at[k], device)
        for k, device in enumerate(mates)
    ]
    load.wait()
    lane = lax.broadcasted_iota(jnp.int32, (cells_y, cells_z), 1)

    def plane(x, acc):
        here = lane == x
        rolled = [
            pltpu.roll(inside[comp, x], lax.rem(x + last, cells_z), 1)
            for last in range(2)
            for comp in (0, 1)
        ]
        return tuple(jnp.where(here, new, old) for new, old in zip(rolled, acc))

    zero = jnp.zeros((cells_y, cells_z), jnp.float32)
    columns = lax.fori_loop(0, cells_x, plane, (zero,) * 4, unroll=4)
    for last in range(2):
        for i in range(2):
            z_faces[last, i] = columns[2 * last + i]
    near, far = plane_order(n_x, n_y, -1)
    for k, (x, y, _) in enumerate(near + far):
        order[k] = x * n_y + y
    own.wait()
    for copy in first:
        copy.wait()
    for k, device in enumerate(peers):
        sem = n_z - 1 + k
        copies.append(
            send_to(near_part, far_part.at[k], part_send.at[sem], part_recv.at[sem], device)
        )
    k = len(moves)
    for src, spot, step in ((1, 4, 1), (0, 5, -1)):
        copies.append(
            send_to(
                z_faces.at[src], halos.at[spot, :, across], send_sem.at[k], recv_sem.at[k],
                beside(2, step),
            )
        )
        k += 1
    for copy in copies:
        copy.wait()
    most = jnp.maximum(jnp.max(near_part[...], axis=0), jnp.max(far_part[...], axis=(0, 1)))
    pair, extra = jnp.max(most[0:1]), jnp.max(most[1:2])
    chosen = jnp.int32(len(tiers) - 1)
    for index in reversed(range(len(tiers) - 1)):
        rows, spill = tiers[index]
        fits = pair <= rows
        if spill:
            fits = jnp.logical_and(fits, extra <= spill)
        chosen = jnp.where(fits, index, chosen)
    tier[0] = chosen


def block_rows(plane):
    cells_y, cells_z = plane.shape
    tiles = plane.reshape(cells_y // BY, BY, cells_z)
    sub = lax.broadcasted_iota(jnp.int32, tiles.shape, 1)
    group = lax.broadcasted_iota(jnp.int32, tiles.shape, 2) // BZ
    k = 1
    while k < BY:
        s_bit, g_bit = (sub & k) != 0, (group & k) != 0
        fwd = pltpu.roll(pltpu.roll(tiles, BY - k, 1), k * BZ, 2)
        back = pltpu.roll(pltpu.roll(tiles, k, 1), cells_z - k * BZ, 2)
        tiles = jnp.where(s_bit == g_bit, tiles, jnp.where(g_bit, fwd, back))
        k *= 2
    return tiles.reshape(cells_y, cells_z)


def blocks_kernel(
    n_x, n_y, region, direct, lists, tallies, blank, vel, halos, table, out, squares, meta, spill,
    starts, coeffs, plan, counts, meta_sem, plan_sem, count_sem,
):
    comps, cells_x, cells_y, cells_z = vel.shape
    nblk = coeffs.shape[0] // comps
    per_plane = nblk // cells_x
    width = out.shape[1]
    row = lax.broadcasted_iota(jnp.int32, (cells_y, cells_z), 0)
    lane = lax.broadcasted_iota(jnp.int32, (cells_y, cells_z), 1)
    clear = pltpu.make_async_copy(blank, meta, meta_sem)
    clear.start()
    fetch = pltpu.make_async_copy(lists, plan, plan_sem)
    fetch.start()
    tally = pltpu.make_async_copy(tallies, counts, count_sem)
    tally.start()

    def plane(x, acc):
        u, v, w = vel[0, x], vel[1, x], vel[2, x]

        def along_x(comp):
            nxt = jnp.where(
                x == cells_x - 1, halos[1, comp - 1, :cells_y], vel[comp, jnp.minimum(x + 1, cells_x - 1)]
            )
            prv = jnp.where(x == 0, halos[0, comp - 1, :cells_y], vel[comp, jnp.maximum(x - 1, 0)])
            return (nxt - prv) * 0.5

        def along_y(f, face):
            nxt = jnp.where(
                row == cells_y - 1, halos[3, face, pl.ds(x, 1), :], pltpu.roll(f, cells_y - 1, 0)
            )
            prv = jnp.where(row == 0, halos[2, face, pl.ds(x, 1), :], pltpu.roll(f, 1, 0))
            return (nxt - prv) * 0.5

        def along_z(f, face):
            after = pltpu.roll(halos[5, face, :cells_y], cells_z - 1 - x, 1)
            before = pltpu.roll(halos[4, face, :cells_y], lax.rem(cells_z - x, cells_z), 1)
            nxt = jnp.where(lane == cells_z - 1, after, pltpu.roll(f, cells_z - 1, 1))
            prv = jnp.where(lane == 0, before, pltpu.roll(f, 1, 1))
            return (nxt - prv) * 0.5

        curl = (
            along_y(w, 1) - along_z(v, 1),
            along_z(u, 0) - along_x(2),
            along_x(1) - along_y(u, 0),
        )
        for c in curl:
            acc = acc + jnp.sum((c * c).reshape(cells_y // 8, 8, cells_z), axis=0)
        flat = jnp.concatenate([block_rows(c) for c in curl], axis=0)
        high = flat.astype(jnp.bfloat16)
        low = (flat - high.astype(jnp.float32)).astype(jnp.bfloat16)
        both = jnp.dot(
            jnp.concatenate([high, low], axis=1), table[...], preferred_element_type=jnp.float32
        )
        result = both[:, :width] + both[:, width:]
        start = x * (comps * per_plane)
        for c in range(comps):
            coeffs[pl.ds(start + c, per_plane, stride=comps), :] = result[
                c * per_plane : (c + 1) * per_plane
            ]
        return acc

    spread = lax.broadcasted_iota(jnp.int32, (comps, width), 1)
    group = 8

    def place(x):
        for start in range(0, per_plane, group):
            found = []
            for k in range(start, min(start + group, per_plane)):
                i = x * per_plane + k
                word = plan[i]
                meta[plan[2 * nblk + i]] = plan[nblk + i]
                shift = word & (width - 1)
                row = lax.shift_right_logical(word, 16)
                moved = pltpu.roll(coeffs[pl.ds(i * comps, comps), :], shift, 1)
                found.append((row, moved, spread >= shift))
            for row, moved, mask in found:
                pltpu.store(out.at[pl.ds(row, comps), :], moved, mask=mask)
                out[pl.ds(row + comps, comps), :] = moved

    together = next(n for n in (UNROLL, 2, 1) if cells_x % n == 0)

    def step(t, acc):
        for k in range(together):
            place((t - 1) * together + k)
        return planes(t, acc)

    def planes(t, acc):
        for k in range(together):
            acc = plane(t * together + k, acc)
        return acc

    clear.wait()
    fetch.wait()
    tally.wait()
    first = planes(0, jnp.zeros((8, cells_z), jnp.float32))
    squares[...] = lax.fori_loop(1, cells_x // together, step, first)
    for k in range(together):
        place(cells_x - together + k)

    half = max(1, n_y // 2)
    facing = lax.rem(lax.div(lax.axis_index("gy"), half) + 1, 2) * half
    most = spill.shape[0] // comps

    def segment(j, begin):
        writer = lax.div(j, half) * n_y + facing + lax.rem(j, half)
        tiles = jnp.minimum(spill_tiles(counts[writer, 0], direct), most - begin)
        starts[j] = begin
        source = (writer * region + direct) * comps

        def tile(i, _):
            for c in range(comps):
                at = source + (i * comps + c) * 8
                spill[(begin + i) * comps + c] = out[pl.ds(pl.multiple_of(at, 8), 8), :]
            return 0

        lax.fori_loop(0, tiles, tile, 0)
        return begin + tiles

    lax.fori_loop(0, n_x * half, segment, jnp.int32(0))


def halves(n_y):
    return n_y if n_y % 2 else n_y // 2


def plane_order(n_x, n_y, sign):
    a, b, c = (lax.axis_index(axis) for axis in ("gx", "gy", "wa"))
    half = halves(n_y)
    mine = lax.rem(b, half)
    base = b - mine
    steps = [(i, j) for i in range(n_x) for j in range(half)]

    def at(base, i, j):
        x = lax.rem(a + sign * i + n_x, n_x)
        return (x, base + lax.rem(mine + sign * j + half, half), c)

    near = [at(base, i, j) for i, j in steps]
    other = lax.rem(base + half, n_y)
    far = [at(other, i, j) for i, j in steps] if half < n_y else []
    return near, far


def unpack(count, marks, source, target, lane, at):
    comps, width = lane.shape
    group = math.gcd(marks[0].shape[-1], 32 if count <= 4 else 4)
    lists, k = marks
    per_line = lists.shape[2] // group

    def some(t, _):
        line = lax.div(t, per_line)
        start = lax.rem(t, per_line) * group
        for i in range(group):
            mark = lists[k, line, start + i]
            fields = jnp.full((comps, width), mark, jnp.int32)
            ahead = lane + (lax.shift_right_logical(fields, 8) & 255)
            row = lax.shift_right_logical(mark, 16)
            head = source[pl.ds(row, comps), :]
            tail = source[pl.ds(row + comps, comps), :]
            joined = jnp.where(ahead >= width, head, tail)
            moved = pltpu.roll(joined, lax.shift_right_logical(mark, 8) & (width - 1), 1)
            value = jnp.where(lane < (fields & 255), moved, 0.0)
            target[at, pl.ds((t * group + i) * comps, comps), :] = value
        return 0

    lax.fori_loop(0, lists.shape[1] * per_line, some, 0)


def exchange_kernel(
    n_x, n_y, n_z, comps, rows, direct, extra, send, squares, meta, spill, starts, total, heard, done,
    near_part, far_part, stage, marks, send_sem, recv_sem, part_send, part_recv, word_send, word_recv,
    own_sem, done_sem, mark_sem, *rest,
):
    c = lax.axis_index("wa")
    near, far = plane_order(n_x, n_y, 1)
    me = near[0][0] * n_y + near[0][1]
    devices = near + far
    held, relay = rest[: len(devices)], rest[len(devices) :]
    half = halves(n_y)
    inner = range(1, len(near))
    outer = sorted(range(len(near), len(devices)), key=lambda k: ((k - len(near)) % half, k))
    mates = line_mates(n_z)
    barrier = pltpu.get_barrier_semaphore()
    for device in mates + devices[1:]:
        pl.semaphore_signal(barrier, inc=1, device_id=device, device_id_type=MESH)
    pl.semaphore_wait(barrier, len(devices) - 1 + len(mates))

    def number(device):
        return device[0] * n_y + device[1]

    whole = pl.ds(0, rows * comps)
    short = pl.ds(0, direct * comps) if extra else whole
    words, blocks, relays, copies = {}, {}, {}, []

    def blocks_to(k):
        used = whole if k < len(near) else short
        blocks[k] = send_to(
            send.at[number(devices[k]), used], held[k].at[used], send_sem.at[k], recv_sem.at[k],
            devices[k],
        )

    own = [
        pltpu.make_async_copy(squares, near_part.at[c], own_sem.at[0]),
        pltpu.make_async_copy(meta.at[me], marks.at[0], mark_sem.at[0]),
        pltpu.make_async_copy(send.at[me, whole], held[0].at[whole], own_sem.at[1]),
    ]
    for copy in own:
        copy.start()
    first = [
        send_to(squares, near_part.at[c], part_send.at[k], part_recv.at[k], device)
        for k, device in enumerate(mates)
    ]
    if extra:
        (
            landed, ready, begins, places, relay_send, relay_recv, spill_send, spill_recv, begin_sem
        ) = relay
        tiles = pl.ds(0, extra * comps // 8)
        poured = [
            send_to(starts, begins, spill_send.at[0], spill_recv.at[0], far[0]),
            send_to(spill.at[tiles], landed.at[tiles], spill_send.at[1], spill_recv.at[1], far[0]),
        ]
    for k in range(1, len(devices)):
        words[k] = send_to(
            meta.at[number(devices[k])], heard.at[k], word_send.at[k], word_recv.at[k], devices[k]
        )
    for k in inner:
        blocks_to(k)
    early = len(outer) // 2 if extra else len(outer)
    for k in outer[:early]:
        blocks_to(k)
    own[0].wait()
    for copy in first:
        copy.wait()
    for k in range(1, len(devices)):
        sem = n_z - 2 + k
        copies.append(
            send_to(near_part, far_part.at[k - 1], part_send.at[sem], part_recv.at[sem], devices[k])
        )
    lane = lax.broadcasted_iota(jnp.int32, (comps, send.shape[2]), 1)

    def place(k):
        if k:
            words[k].wait()
            load = pltpu.make_async_copy(heard.at[k], marks.at[k], mark_sem.at[k])
            load.start()
            blocks[k].wait()
            if k in relays:
                relays[k].wait()
            load.wait()
        else:
            own[1].wait()
            own[2].wait()
        unpack(len(near), (marks, k), held[k], stage, lane, k)
        out = pltpu.make_async_copy(stage.at[k], done.at[k], done_sem.at[k])
        out.start()
        copies.append(out)

    place(0)
    if extra:
        poured[0].wait()
        load = pltpu.make_async_copy(begins, places, begin_sem.at[0])
        load.start()
        load.wait()
        poured[1].wait()
        size = (rows - direct) * comps
        for k, (x, y, _) in enumerate(near):
            begin = places[0, x * half + lax.rem(y, half)] * comps

            def tile(i, _, k=k, begin=begin):
                ready[k, pl.ds(pl.multiple_of(i * 8, 8), 8), :] = landed[begin + i]
                return 0

            lax.fori_loop(0, size // 8, tile, 0)
        past = pl.ds(direct * comps, size)
        for k, device in enumerate(near):
            target = held[len(near) + k].at[past]
            if k:
                relays[len(near) + k] = send_to(
                    ready.at[k], target, relay_send.at[k], relay_recv.at[k], device
                )
            else:
                def keep(i, _):
                    at = pl.ds(pl.multiple_of(i * 8, 8), 8)
                    held[len(near)][pl.ds(pl.multiple_of(direct * comps + i * 8, 8), 8), :] = ready[
                        0, at, :
                    ]
                    return 0

                lax.fori_loop(0, size // 8, keep, 0)
    for k in outer[early:]:
        blocks_to(k)
    for k in inner:
        place(k)
    for k in outer:
        place(k)
    for copy in copies:
        copy.wait()
    total[...] = jnp.sum(near_part[...], axis=0) + jnp.sum(far_part[...], axis=(0, 1))


def finish_kernel(every, order, squares, done, out, scale):
    comps, _, capacity, width = out.shape

    @pl.when(pl.program_id(0) == 0)
    def _():
        total = jnp.sum(squares[...], keepdims=True)
        scale[...] = jnp.broadcast_to(1.0 / jnp.sqrt(total / every + 1e-06), scale.shape)

    for c in range(comps):
        out[c, 0] = done[0, pl.ds(c, capacity, stride=comps), :] * scale[:1]


def tier_sizes(capacity, n_y):
    def up(part):
        return -(-capacity * part // (64 * 8)) * 8

    direct = [(up(part), 0) for part in (52, 64)]
    if n_y % 2:
        return up(64), direct
    parts = ((38, 28), (39, 36), (39, 44), (40, 54))
    spilled = [(up(rows), up(extra)) for rows, extra in parts]
    return up(18), spilled + direct


def local(velocity, lengths, destinations):
    n_x, n_y, n_z = lax.axis_size("gx"), lax.axis_size("gy"), lax.axis_size("wa")
    comps, cells_x, cells_y, cells_z = velocity.shape
    width = BY * BZ
    nblk = cells_x * cells_y * cells_z // width
    writers = n_x * n_y
    capacity = max(2, 2 * nblk // writers)
    region = capacity + 8
    f32 = jnp.float32
    direct, tiers = tier_sizes(capacity, n_y)
    most_extra = max([8] + [extra for _, extra in tiers])
    senders = n_x * halves(n_y)

    smem = pl.BlockSpec(memory_space=pltpu.SMEM)
    vmem = pl.BlockSpec(memory_space=pltpu.VMEM)
    anywhere = pl.BlockSpec(memory_space=pl.ANY)
    dma = pltpu.SemaphoreType.DMA
    plan, tallies, inside, halos, tier, order = pl.pallas_call(
        functools.partial(front_kernel, (n_x, n_y, n_z), tiers, capacity, region, direct),
        out_shape=(
            jax.ShapeDtypeStruct((3, nblk // 128, 128), jnp.int32),
            jax.ShapeDtypeStruct((writers, 128), jnp.int32),
            jax.ShapeDtypeStruct(velocity.shape, f32),
            jax.ShapeDtypeStruct((6, 2, max(cells_x, cells_y), cells_z), f32),
            jax.ShapeDtypeStruct((1,), jnp.int32),
            jax.ShapeDtypeStruct((writers,), jnp.int32),
        ),
        in_specs=[vmem, vmem, anywhere],
        out_specs=(vmem, vmem, vmem, vmem, smem, smem),
        scratch_shapes=[
            pltpu.VMEM((2, 2, cells_y, cells_z), f32),
            pltpu.VMEM((8, 128), f32),
            pltpu.VMEM((writers, 128), f32),
            pltpu.VMEM((n_z, 8, 128), f32),
            pltpu.VMEM((writers - 1, n_z, 8, 128), f32),
            dma((8,)),
            dma((8,)),
            dma((writers + n_z - 2,)),
            dma((writers + n_z - 2,)),
            dma((2,)),
        ],
        compiler_params=pltpu.CompilerParams(
            collective_id=1, has_side_effects=True, vmem_limit_bytes=50 * 2**20
        ),
        name="front",
    )(destinations.reshape(nblk // 128, 128), lengths.reshape(nblk // 128, 128), velocity)

    table = jnp.asarray(split_table())
    outgoing, squares, meta, spill, starts = pl.pallas_call(
        functools.partial(blocks_kernel, n_x, n_y, region, direct),
        out_shape=(
            jax.ShapeDtypeStruct((writers * region * comps, width), f32),
            jax.ShapeDtypeStruct((8, cells_z), f32),
            jax.ShapeDtypeStruct((writers * capacity,), jnp.int32),
            jax.ShapeDtypeStruct((most_extra * comps // 8, 8, width), f32),
            jax.ShapeDtypeStruct((128,), jnp.int32),
        ),
        in_specs=[anywhere] * 3 + [vmem] * 3,
        out_specs=(vmem, vmem, smem, vmem, smem),
        scratch_shapes=[
            pltpu.VMEM((nblk * comps, width), f32),
            pltpu.SMEM((3 * nblk,), jnp.int32),
            pltpu.SMEM((writers, 128), jnp.int32),
            dma,
            dma,
            dma,
        ],
        compiler_params=pltpu.CompilerParams(vmem_limit_bytes=48 * 2**20),
        name="blocks",
    )(
        plan.reshape(3 * nblk),
        tallies,
        jnp.zeros((writers * capacity,), jnp.int32),
        inside,
        halos,
        table,
    )
    outgoing = outgoing.reshape(writers, region * comps, width)
    part = min(capacity, 128)
    meta = meta.reshape(writers, capacity // part, part)

    def exchange(index, *operands):
        rows, extra = tiers[index]
        size = (rows - direct) * comps
        held = [pltpu.VMEM(((rows + 8) * comps, width), f32) for _ in range(writers)]
        relay = [
            pltpu.VMEM(((extra * comps + size) // 8, 8, width), f32),
            pltpu.VMEM((senders, size, width), f32),
            pltpu.VMEM((1, 128), jnp.int32),
            pltpu.SMEM((1, 128), jnp.int32),
            dma((senders,)),
            dma((senders,)),
            dma((2,)),
            dma((2,)),
            dma((2,)),
        ]
        return pl.pallas_call(
            functools.partial(exchange_kernel, n_x, n_y, n_z, comps, rows, direct, extra),
            out_shape=(
                jax.ShapeDtypeStruct(squares.shape, f32),
                jax.ShapeDtypeStruct(meta.shape, jnp.int32),
                jax.ShapeDtypeStruct((writers, capacity * comps, width), f32),
            ),
            in_specs=[anywhere, vmem, anywhere, anywhere, anywhere],
            out_specs=(vmem, anywhere, anywhere),
            scratch_shapes=[
                pltpu.VMEM((n_z,) + squares.shape, f32),
                pltpu.VMEM((writers - 1, n_z) + squares.shape, f32),
                pltpu.VMEM((writers, capacity * comps, width), f32),
                pltpu.SMEM(meta.shape, jnp.int32),
                dma((writers,)),
                dma((writers,)),
                dma((writers + n_z - 2,)),
                dma((writers + n_z - 2,)),
                dma((writers,)),
                dma((writers,)),
                dma((2,)),
                dma((writers,)),
                dma((writers,)),
            ]
            + held
            + (relay if extra else []),
            compiler_params=pltpu.CompilerParams(
                collective_id=2 + index, has_side_effects=True, vmem_limit_bytes=48 * 2**20
            ),
            name=f"exchange{rows}_{extra}",
        )(*operands)

    branches = [functools.partial(exchange, index) for index in range(len(tiers))]
    squares, heard, done = lax.switch(
        tier[0], branches, outgoing, squares, meta, spill, starts.reshape(1, 128)
    )

    every = velocity.size * n_x * n_y * n_z
    received = pl.pallas_call(
        functools.partial(finish_kernel, float(every)),
        grid_spec=pltpu.PrefetchScalarGridSpec(
            num_scalar_prefetch=1,
            grid=(writers,),
            in_specs=[
                pl.BlockSpec((8, cells_z), lambda s, order: (0, 0)),
                pl.BlockSpec((1, capacity * comps, width), lambda s, order: (s, 0, 0)),
            ],
            out_specs=pl.BlockSpec(
                (comps, 1, capacity, width), lambda s, order: (0, order[s], 0, 0)
            ),
            scratch_shapes=[pltpu.VMEM((8, width), f32)],
        ),
        out_shape=jax.ShapeDtypeStruct((comps, writers, capacity, width), f32),
        name="finish",
    )(order, squares, done)
    return received.reshape(1, 1, comps, writers, capacity, width)


def solution(mesh):
    return jax.shard_map(
        local,
        mesh=mesh,
        in_specs=(
            P(None, "gx", "gy", "wa"),
            P("gx", "gy", "wa", None),
            P("gx", "gy", "wa", None, None),
        ),
        out_specs=P(("gx", "gy"), "wa", None, None, None, None),
        check_vma=False,
    )
```

```python
import functools
import math

import jax
import jax.numpy as jnp
import numpy as np
from jax import lax
from jax.experimental import pallas as pl
from jax.experimental.pallas import tpu as pltpu
from jax.sharding import PartitionSpec as P

BY = 8
BZ = 16
UNROLL = 2
MESH = pl.DeviceIdType.MESH


def dct_table(count):
    freqs, points = np.arange(count)[:, None], np.arange(count)[None, :]
    table = np.cos(np.pi * (points + 0.5) * freqs / count) * np.sqrt(2.0 / count)
    return np.where(freqs == 0, table * np.sqrt(0.5), table)


def split_table():
    kron = np.kron(dct_table(BY), dct_table(BZ)).T.astype(np.float32)
    high = kron.astype(jnp.bfloat16)
    low = (kron - high.astype(np.float32)).astype(jnp.bfloat16)
    return np.block([[high, low], [high, np.zeros_like(low)]]).astype(jnp.bfloat16)


def spill_tiles(used, direct):
    return lax.shift_right_logical(jnp.maximum(used - direct, 0) + 7, 3)


def plan_blocks(writers, capacity, region, direct, n_y, comps, t, kept, plan, counts, need, sums):
    rows, lanes = t.shape
    shape = (lanes, lanes)
    upper = (
        lax.broadcasted_iota(jnp.int32, shape, 0) < lax.broadcasted_iota(jnp.int32, shape, 1)
    ).astype(jnp.float32).astype(jnp.bfloat16)
    square = (rows, rows)
    lower = (
        lax.broadcasted_iota(jnp.int32, square, 1) < lax.broadcasted_iota(jnp.int32, square, 0)
    ).astype(jnp.float32).astype(jnp.bfloat16)
    weight = kept.astype(jnp.float32)

    def body(w, acc):
        spot, start, site = acc
        mine = t == w
        ones = mine.astype(jnp.float32)
        sizes = jnp.where(mine, weight, 0.0)
        both = jnp.concatenate([ones, sizes], axis=0).astype(jnp.bfloat16)
        sums[pl.ds(w, 1), :] = jnp.sum(sizes, axis=0, keepdims=True)
        inner = jnp.dot(both, upper, preferred_element_type=jnp.float32)
        side = jnp.concatenate([ones, sizes], axis=1).astype(jnp.bfloat16)
        before = jnp.dot(lower, side, preferred_element_type=jnp.float32)
        rank = inner[:rows] + jnp.sum(before[:, :lanes], axis=1, keepdims=True)
        offset = inner[rows:] + jnp.sum(before[:, lanes:], axis=1, keepdims=True)
        spot = jnp.where(mine, w * capacity + rank.astype(jnp.int32), spot)
        offset = offset.astype(jnp.int32)
        start = jnp.where(mine, offset, start)
        site = jnp.where(mine, w * region, site)
        return spot, start, site

    none = jnp.zeros_like(t)
    spot, start, site = lax.fori_loop(0, writers, body, (none, none, none), unroll=8)
    used = jnp.sum(sums[...], axis=1, keepdims=True).astype(jnp.int32)
    used = jnp.broadcast_to(lax.shift_right_logical(used + (lanes - 1), 7), counts.shape)
    counts[...] = used
    writer = lax.broadcasted_iota(jnp.int32, counts.shape, 0)
    half = max(1, n_y // 2)
    far_side = lax.div(lax.rem(writer, n_y), half) != lax.div(lax.axis_index("gy"), half)
    over = jnp.where(far_side, spill_tiles(used, direct) * 8, 0)
    most = jnp.max(used.astype(jnp.float32), axis=0, keepdims=True)
    extra = jnp.sum(over.astype(jnp.float32), axis=0, keepdims=True)
    line = lax.broadcasted_iota(jnp.int32, need.shape, 0)
    need[...] = jnp.where(line == 0, most, jnp.where(line == 1, extra, 0.0))
    shift = start & (lanes - 1)
    row = lax.shift_right_logical(start, lanes.bit_length() - 1)
    plan[2] = spot
    plan[0] = (row + site) * (comps << 16) + shift
    plan[1] = row * (comps << 16) + (lanes - shift) * 256 + kept


def plane_offsets(n_x, n_y):
    offsets = [(i, j) for i in range(n_x) for j in range(n_y) if i or j]
    return sorted(offsets, key=lambda o: (bool(o[0]) and bool(o[1]), min(o[1], n_y - o[1])))


def plane_peers(n_x, n_y):
    a, b, c = (lax.axis_index(axis) for axis in ("gx", "gy", "wa"))
    return [(lax.rem(a + i, n_x), lax.rem(b + j, n_y), c) for i, j in plane_offsets(n_x, n_y)]


def line_mates(n_z):
    a, b, c = (lax.axis_index(axis) for axis in ("gx", "gy", "wa"))
    return [(a, b, lax.rem(c + k, n_z)) for k in range(1, n_z)]


def send_to(src, dst, send_sem, recv_sem, device):
    copy = pltpu.make_async_remote_copy(
        src_ref=src,
        dst_ref=dst,
        send_sem=send_sem,
        recv_sem=recv_sem,
        device_id=device,
        device_id_type=MESH,
    )
    copy.start()
    return copy


def spill_tiles(used, direct):
    return lax.shift_right_logical(jnp.maximum(used - direct, 0) + 7, 3)


def front_kernel(
    sizes, tiers, capacity, region, direct, targets, lens, vel, plan, counts, inside, halos, tier,
    z_faces, need, sums, near_part, far_part, send_sem, recv_sem, part_send, part_recv, own_sem,
):
    place = [lax.axis_index(axis) for axis in ("gx", "gy", "wa")]
    n_x, n_y, n_z = sizes
    comps, cells_x, cells_y, cells_z = vel.shape
    writers = n_x * n_y
    load = pltpu.make_async_copy(vel, inside, own_sem.at[0])
    load.start()

    def beside(axis, step):
        size = sizes[axis]
        moved = lax.rem(place[axis] + step + size, size)
        return tuple(moved if i == axis else p for i, p in enumerate(place))

    across, along = pl.ds(0, cells_y), pl.ds(0, cells_x)
    peers, mates = plane_peers(n_x, n_y), line_mates(n_z)
    others = [beside(axis, step) for axis in range(3) for step in (1, -1)] + peers + mates
    barrier = pltpu.get_barrier_semaphore()
    for device in others:
        pl.semaphore_signal(barrier, inc=1, device_id=device, device_id_type=MESH)
    plan_blocks(
        writers, capacity, region, direct, n_y, comps, targets[...], lens[...], plan, counts, need,
        sums,
    )
    pl.semaphore_wait(barrier, len(others))
    moves = [
        (vel.at[pl.ds(1, 2), cells_x - 1], halos.at[0, :, across], beside(0, 1)),
        (vel.at[pl.ds(1, 2), 0], halos.at[1, :, across], beside(0, -1)),
    ]
    for i, comp in enumerate((0, 2)):
        moves += [
            (vel.at[comp, :, cells_y - 1], halos.at[2, i, along], beside(1, 1)),
            (vel.at[comp, :, 0], halos.at[3, i, along], beside(1, -1)),
        ]
    copies = [
        send_to(src, dst, send_sem.at[k], recv_sem.at[k], device)
        for k, (src, dst, device) in enumerate(moves)
    ]
    c = place[2]
    own = pltpu.make_async_copy(need, near_part.at[c], own_sem.at[1])
    own.start()
    first = [
        send_to(need, near_part.at[c], part_send.at[k], part_recv.at[k], device)
        for k, device in enumerate(mates)
    ]
    load.wait()
    lane = lax.broadcasted_iota(jnp.int32, (cells_y, cells_z), 1)

    def plane(x, acc):
        here = lane == x
        rolled = [
            pltpu.roll(inside[comp, x], lax.rem(x + last, cells_z), 1)
            for last in range(2)
            for comp in (0, 1)
        ]
        return tuple(jnp.where(here, new, old) for new, old in zip(rolled, acc))

    zero = jnp.zeros((cells_y, cells_z), jnp.float32)
    columns = lax.fori_loop(0, cells_x, plane, (zero,) * 4, unroll=4)
    for last in range(2):
        for i in range(2):
            z_faces[last, i] = columns[2 * last + i]
    own.wait()
    for copy in first:
        copy.wait()
    for k, device in enumerate(peers):
        sem = n_z - 1 + k
        copies.append(
            send_to(near_part, far_part.at[k], part_send.at[sem], part_recv.at[sem], device)
        )
    k = len(moves)
    for src, spot, step in ((1, 4, 1), (0, 5, -1)):
        copies.append(
            send_to(
                z_faces.at[src], halos.at[spot, :, across], send_sem.at[k], recv_sem.at[k],
                beside(2, step),
            )
        )
        k += 1
    for copy in copies:
        copy.wait()
    most = jnp.maximum(jnp.max(near_part[...], axis=0), jnp.max(far_part[...], axis=(0, 1)))
    pair, extra = jnp.max(most[0:1]), jnp.max(most[1:2])
    chosen = jnp.int32(len(tiers) - 1)
    for index in reversed(range(len(tiers) - 1)):
        rows, spill = tiers[index]
        fits = pair <= rows
        if spill:
            fits = jnp.logical_and(fits, extra <= spill)
        chosen = jnp.where(fits, index, chosen)
    tier[0] = chosen


def block_rows(plane):
    cells_y, cells_z = plane.shape
    tiles = plane.reshape(cells_y // BY, BY, cells_z)
    sub = lax.broadcasted_iota(jnp.int32, tiles.shape, 1)
    group = lax.broadcasted_iota(jnp.int32, tiles.shape, 2) // BZ
    k = 1
    while k < BY:
        s_bit, g_bit = (sub & k) != 0, (group & k) != 0
        fwd = pltpu.roll(pltpu.roll(tiles, BY - k, 1), k * BZ, 2)
        back = pltpu.roll(pltpu.roll(tiles, k, 1), cells_z - k * BZ, 2)
        tiles = jnp.where(s_bit == g_bit, tiles, jnp.where(g_bit, fwd, back))
        k *= 2
    return tiles.reshape(cells_y, cells_z)


def blocks_kernel(
    n_x, n_y, region, direct, lists, tallies, blank, vel, halos, table, out, squares, meta, spill,
    starts, coeffs, plan, counts, meta_sem, plan_sem, count_sem,
):
    comps, cells_x, cells_y, cells_z = vel.shape
    nblk = coeffs.shape[0] // comps
    per_plane = nblk // cells_x
    width = out.shape[1]
    row = lax.broadcasted_iota(jnp.int32, (cells_y, cells_z), 0)
    lane = lax.broadcasted_iota(jnp.int32, (cells_y, cells_z), 1)
    clear = pltpu.make_async_copy(blank, meta, meta_sem)
    clear.start()
    fetch = pltpu.make_async_copy(lists, plan, plan_sem)
    fetch.start()
    tally = pltpu.make_async_copy(tallies, counts, count_sem)
    tally.start()

    def plane(x, acc):
        u, v, w = vel[0, x], vel[1, x], vel[2, x]

        def along_x(comp):
            nxt = jnp.where(
                x == cells_x - 1, halos[1, comp - 1, :cells_y], vel[comp, jnp.minimum(x + 1, cells_x - 1)]
            )
            prv = jnp.where(x == 0, halos[0, comp - 1, :cells_y], vel[comp, jnp.maximum(x - 1, 0)])
            return (nxt - prv) * 0.5

        def along_y(f, face):
            nxt = jnp.where(
                row == cells_y - 1, halos[3, face, pl.ds(x, 1), :], pltpu.roll(f, cells_y - 1, 0)
            )
            prv = jnp.where(row == 0, halos[2, face, pl.ds(x, 1), :], pltpu.roll(f, 1, 0))
            return (nxt - prv) * 0.5

        def along_z(f, face):
            after = pltpu.roll(halos[5, face, :cells_y], cells_z - 1 - x, 1)
            before = pltpu.roll(halos[4, face, :cells_y], lax.rem(cells_z - x, cells_z), 1)
            nxt = jnp.where(lane == cells_z - 1, after, pltpu.roll(f, cells_z - 1, 1))
            prv = jnp.where(lane == 0, before, pltpu.roll(f, 1, 1))
            return (nxt - prv) * 0.5

        curl = (
            along_y(w, 1) - along_z(v, 1),
            along_z(u, 0) - along_x(2),
            along_x(1) - along_y(u, 0),
        )
        for c in curl:
            acc = acc + jnp.sum((c * c).reshape(cells_y // 8, 8, cells_z), axis=0)
        flat = jnp.concatenate([block_rows(c) for c in curl], axis=0)
        high = flat.astype(jnp.bfloat16)
        low = (flat - high.astype(jnp.float32)).astype(jnp.bfloat16)
        both = jnp.dot(
            jnp.concatenate([high, low], axis=1), table[...], preferred_element_type=jnp.float32
        )
        result = both[:, :width] + both[:, width:]
        start = x * (comps * per_plane)
        for c in range(comps):
            coeffs[pl.ds(start + c, per_plane, stride=comps), :] = result[
                c * per_plane : (c + 1) * per_plane
            ]
        return acc

    spread = lax.broadcasted_iota(jnp.int32, (comps, width), 1)
    group = 8

    def place(x):
        for start in range(0, per_plane, group):
            found = []
            for k in range(start, min(start + group, per_plane)):
                i = x * per_plane + k
                word = plan[i]
                meta[plan[2 * nblk + i]] = plan[nblk + i]
                shift = word & (width - 1)
                row = lax.shift_right_logical(word, 16)
                moved = pltpu.roll(coeffs[pl.ds(i * comps, comps), :], shift, 1)
                found.append((row, moved, spread >= shift))
            for row, moved, mask in found:
                pltpu.store(out.at[pl.ds(row, comps), :], moved, mask=mask)
                out[pl.ds(row + comps, comps), :] = moved

    together = next(n for n in (UNROLL, 2, 1) if cells_x % n == 0)

    def step(t, acc):
        for k in range(together):
            place((t - 1) * together + k)
        return planes(t, acc)

    def planes(t, acc):
        for k in range(together):
            acc = plane(t * together + k, acc)
        return acc

    clear.wait()
    fetch.wait()
    tally.wait()
    first = planes(0, jnp.zeros((8, cells_z), jnp.float32))
    squares[...] = lax.fori_loop(1, cells_x // together, step, first)
    for k in range(together):
        place(cells_x - together + k)

    half = max(1, n_y // 2)
    facing = lax.rem(lax.div(lax.axis_index("gy"), half) + 1, 2) * half
    most = spill.shape[0] // comps

    def segment(j, begin):
        writer = lax.div(j, half) * n_y + facing + lax.rem(j, half)
        tiles = jnp.minimum(spill_tiles(counts[writer, 0], direct), most - begin)
        starts[j] = begin
        source = (writer * region + direct) * comps

        def tile(i, _):
            for c in range(comps):
                at = source + (i * comps + c) * 8
                spill[(begin + i) * comps + c] = out[pl.ds(pl.multiple_of(at, 8), 8), :]
            return 0

        lax.fori_loop(0, tiles, tile, 0)
        return begin + tiles

    lax.fori_loop(0, n_x * half, segment, jnp.int32(0))


def halves(n_y):
    return n_y if n_y % 2 else n_y // 2


def plane_order(n_x, n_y, sign):
    a, b, c = (lax.axis_index(axis) for axis in ("gx", "gy", "wa"))
    half = halves(n_y)
    mine = lax.rem(b, half)
    base = b - mine
    steps = [(i, j) for i in range(n_x) for j in range(half)]

    def at(base, i, j):
        x = lax.rem(a + sign * i + n_x, n_x)
        return (x, base + lax.rem(mine + sign * j + half, half), c)

    near = [at(base, i, j) for i, j in steps]
    other = lax.rem(base + half, n_y)
    far = [at(other, i, j) for i, j in steps] if half < n_y else []
    return near, far


def unpack(count, marks, source, target, lane, at):
    comps, width = lane.shape
    group = math.gcd(marks[0].shape[-1], 64 if count <= 4 else 4)
    lists, k = marks
    per_line = lists.shape[2] // group

    def some(t, _):
        line = lax.div(t, per_line)
        start = lax.rem(t, per_line) * group
        for i in range(group):
            mark = lists[k, line, start + i]
            fields = jnp.full((comps, width), mark, jnp.int32)
            ahead = lane + (lax.shift_right_logical(fields, 8) & 255)
            row = lax.shift_right_logical(mark, 16)
            head = source[pl.ds(row, comps), :]
            tail = source[pl.ds(row + comps, comps), :]
            joined = jnp.where(ahead >= width, head, tail)
            moved = pltpu.roll(joined, lax.shift_right_logical(mark, 8) & (width - 1), 1)
            value = jnp.where(lane < (fields & 255), moved, 0.0)
            target[at, pl.ds((t * group + i) * comps, comps), :] = value
        return 0

    lax.fori_loop(0, lists.shape[1] * per_line, some, 0)


def exchange_kernel(
    n_x, n_y, n_z, comps, rows, direct, extra, send, squares, meta, spill, starts, total, heard, done,
    near_part, far_part, stage, marks, send_sem, recv_sem, part_send, part_recv, word_send, word_recv,
    own_sem, done_sem, mark_sem, *rest,
):
    c = lax.axis_index("wa")
    near, far = plane_order(n_x, n_y, 1)
    me = near[0][0] * n_y + near[0][1]
    devices = near + far
    sources = sum(plane_order(n_x, n_y, -1), [])
    held, relay = rest[: len(devices)], rest[len(devices) :]
    half = halves(n_y)
    inner = range(1, len(near))
    outer = sorted(range(len(near), len(devices)), key=lambda k: ((k - len(near)) % half, k))
    mates = line_mates(n_z)
    barrier = pltpu.get_barrier_semaphore()
    for device in mates + devices[1:]:
        pl.semaphore_signal(barrier, inc=1, device_id=device, device_id_type=MESH)
    pl.semaphore_wait(barrier, len(devices) - 1 + len(mates))

    def number(device):
        return device[0] * n_y + device[1]

    whole = pl.ds(0, rows * comps)
    short = pl.ds(0, direct * comps) if extra else whole
    words, blocks, relays, copies = {}, {}, {}, []

    def blocks_to(k):
        used = whole if k < len(near) else short
        blocks[k] = send_to(
            send.at[number(devices[k]), used], held[k].at[used], send_sem.at[k], recv_sem.at[k],
            devices[k],
        )

    own = [
        pltpu.make_async_copy(squares, near_part.at[c], own_sem.at[0]),
        pltpu.make_async_copy(meta.at[me], marks.at[0], mark_sem.at[0]),
        pltpu.make_async_copy(send.at[me, whole], held[0].at[whole], own_sem.at[1]),
    ]
    for copy in own:
        copy.start()
    first = [
        send_to(squares, near_part.at[c], part_send.at[k], part_recv.at[k], device)
        for k, device in enumerate(mates)
    ]
    if extra:
        (
            landed, ready, begins, places, relay_send, relay_recv, spill_send, spill_recv, begin_sem
        ) = relay
        tiles = pl.ds(0, extra * comps // 8)
        poured = [
            send_to(starts, begins, spill_send.at[0], spill_recv.at[0], far[0]),
            send_to(spill.at[tiles], landed.at[tiles], spill_send.at[1], spill_recv.at[1], far[0]),
        ]
    for k in range(1, len(devices)):
        words[k] = send_to(
            meta.at[number(devices[k])], heard.at[k], word_send.at[k], word_recv.at[k], devices[k]
        )
    for k in list(inner) + list(outer):
        blocks_to(k)
    own[0].wait()
    for copy in first:
        copy.wait()
    for k in range(1, len(devices)):
        sem = n_z - 2 + k
        copies.append(
            send_to(near_part, far_part.at[k - 1], part_send.at[sem], part_recv.at[sem], devices[k])
        )
    lane = lax.broadcasted_iota(jnp.int32, (comps, send.shape[2]), 1)

    def place(k):
        if k:
            words[k].wait()
            load = pltpu.make_async_copy(heard.at[k], marks.at[k], mark_sem.at[k])
            load.start()
            blocks[k].wait()
            if k in relays:
                relays[k].wait()
            load.wait()
        else:
            own[1].wait()
            own[2].wait()
        unpack(len(near), (marks, k), held[k], stage, lane, k)
        spot = sources[k][0] * n_y + sources[k][1]
        out = pltpu.make_async_copy(stage.at[k], done.at[spot], done_sem.at[k])
        out.start()
        copies.append(out)

    place(0)
    if extra:
        poured[0].wait()
        load = pltpu.make_async_copy(begins, places, begin_sem.at[0])
        load.start()
        load.wait()
        poured[1].wait()
        size = (rows - direct) * comps
        for k, (x, y, _) in enumerate(near):
            begin = places[0, x * half + lax.rem(y, half)] * comps

            def tile(i, _, k=k, begin=begin):
                ready[k, pl.ds(pl.multiple_of(i * 8, 8), 8), :] = landed[begin + i]
                return 0

            lax.fori_loop(0, size // 8, tile, 0)
        past = pl.ds(direct * comps, size)
        for k, device in enumerate(near):
            target = held[len(near) + k].at[past]
            if k:
                relays[len(near) + k] = send_to(
                    ready.at[k], target, relay_send.at[k], relay_recv.at[k], device
                )
            else:
                def keep(i, _):
                    at = pl.ds(pl.multiple_of(i * 8, 8), 8)
                    held[len(near)][pl.ds(pl.multiple_of(direct * comps + i * 8, 8), 8), :] = ready[
                        0, at, :
                    ]
                    return 0

                lax.fori_loop(0, size // 8, keep, 0)
    for k in inner:
        place(k)
    for k in outer:
        place(k)
    for copy in copies:
        copy.wait()
    total[...] = jnp.sum(near_part[...], axis=0) + jnp.sum(far_part[...], axis=(0, 1))


def finish_kernel(every, squares, done, out, scale):
    comps, together, capacity, width = out.shape

    @pl.when(pl.program_id(0) == 0)
    def _():
        total = jnp.sum(squares[...], keepdims=True)
        scale[...] = jnp.broadcast_to(1.0 / jnp.sqrt(total / every + 1e-06), scale.shape)

    for k in range(together):
        for c in range(comps):
            out[c, k] = done[k, pl.ds(c, capacity, stride=comps), :] * scale[:1]


def tier_sizes(capacity, n_y):
    def up(part):
        return -(-capacity * part // (64 * 8)) * 8

    direct = [(up(part), 0) for part in (64,)]
    if n_y % 2:
        return up(64), direct
    parts = ((38, 28), (39, 36), (39, 44), (40, 54))
    spilled = [(up(rows), up(extra)) for rows, extra in parts]
    return up(18), spilled + direct


def local(velocity, lengths, destinations):
    n_x, n_y, n_z = lax.axis_size("gx"), lax.axis_size("gy"), lax.axis_size("wa")
    comps, cells_x, cells_y, cells_z = velocity.shape
    width = BY * BZ
    nblk = cells_x * cells_y * cells_z // width
    writers = n_x * n_y
    capacity = max(2, 2 * nblk // writers)
    region = capacity + 8
    f32 = jnp.float32
    direct, tiers = tier_sizes(capacity, n_y)
    most_extra = max([8] + [extra for _, extra in tiers])
    senders = n_x * halves(n_y)

    smem = pl.BlockSpec(memory_space=pltpu.SMEM)
    vmem = pl.BlockSpec(memory_space=pltpu.VMEM)
    anywhere = pl.BlockSpec(memory_space=pl.ANY)
    dma = pltpu.SemaphoreType.DMA
    plan, tallies, inside, halos, tier = pl.pallas_call(
        functools.partial(front_kernel, (n_x, n_y, n_z), tiers, capacity, region, direct),
        out_shape=(
            jax.ShapeDtypeStruct((3, nblk // 128, 128), jnp.int32),
            jax.ShapeDtypeStruct((writers, 128), jnp.int32),
            jax.ShapeDtypeStruct(velocity.shape, f32),
            jax.ShapeDtypeStruct((6, 2, max(cells_x, cells_y), cells_z), f32),
            jax.ShapeDtypeStruct((1,), jnp.int32),
        ),
        in_specs=[vmem, vmem, anywhere],
        out_specs=(vmem, vmem, vmem, vmem, smem),
        scratch_shapes=[
            pltpu.VMEM((2, 2, cells_y, cells_z), f32),
            pltpu.VMEM((8, 128), f32),
            pltpu.VMEM((writers, 128), f32),
            pltpu.VMEM((n_z, 8, 128), f32),
            pltpu.VMEM((writers - 1, n_z, 8, 128), f32),
            dma((8,)),
            dma((8,)),
            dma((writers + n_z - 2,)),
            dma((writers + n_z - 2,)),
            dma((2,)),
        ],
        compiler_params=pltpu.CompilerParams(
            collective_id=1, has_side_effects=True, vmem_limit_bytes=50 * 2**20
        ),
        name="front",
    )(destinations.reshape(nblk // 128, 128), lengths.reshape(nblk // 128, 128), velocity)

    table = jnp.asarray(split_table())
    outgoing, squares, meta, spill, starts = pl.pallas_call(
        functools.partial(blocks_kernel, n_x, n_y, region, direct),
        out_shape=(
            jax.ShapeDtypeStruct((writers * region * comps, width), f32),
            jax.ShapeDtypeStruct((8, cells_z), f32),
            jax.ShapeDtypeStruct((writers * capacity,), jnp.int32),
            jax.ShapeDtypeStruct((most_extra * comps // 8, 8, width), f32),
            jax.ShapeDtypeStruct((128,), jnp.int32),
        ),
        in_specs=[anywhere] * 3 + [vmem] * 3,
        out_specs=(vmem, vmem, smem, vmem, smem),
        scratch_shapes=[
            pltpu.VMEM((nblk * comps, width), f32),
            pltpu.SMEM((3 * nblk,), jnp.int32),
            pltpu.SMEM((writers, 128), jnp.int32),
            dma,
            dma,
            dma,
        ],
        compiler_params=pltpu.CompilerParams(vmem_limit_bytes=48 * 2**20),
        name="blocks",
    )(
        plan.reshape(3 * nblk),
        tallies,
        jnp.zeros((writers * capacity,), jnp.int32),
        inside,
        halos,
        table,
    )
    outgoing = outgoing.reshape(writers, region * comps, width)
    part = min(capacity, 128)
    meta = meta.reshape(writers, capacity // part, part)

    def exchange(index, *operands):
        rows, extra = tiers[index]
        size = (rows - direct) * comps
        held = [pltpu.VMEM(((rows + 8) * comps, width), f32) for _ in range(writers)]
        relay = [
            pltpu.VMEM(((extra * comps + size) // 8, 8, width), f32),
            pltpu.VMEM((senders, size, width), f32),
            pltpu.VMEM((1, 128), jnp.int32),
            pltpu.SMEM((1, 128), jnp.int32),
            dma((senders,)),
            dma((senders,)),
            dma((2,)),
            dma((2,)),
            dma((2,)),
        ]
        return pl.pallas_call(
            functools.partial(exchange_kernel, n_x, n_y, n_z, comps, rows, direct, extra),
            out_shape=(
                jax.ShapeDtypeStruct(squares.shape, f32),
                jax.ShapeDtypeStruct(meta.shape, jnp.int32),
                jax.ShapeDtypeStruct((writers, capacity * comps, width), f32),
            ),
            in_specs=[anywhere, vmem, anywhere, anywhere, anywhere],
            out_specs=(vmem, anywhere, anywhere),
            scratch_shapes=[
                pltpu.VMEM((n_z,) + squares.shape, f32),
                pltpu.VMEM((writers - 1, n_z) + squares.shape, f32),
                pltpu.VMEM((writers, capacity * comps, width), f32),
                pltpu.SMEM(meta.shape, jnp.int32),
                dma((writers,)),
                dma((writers,)),
                dma((writers + n_z - 2,)),
                dma((writers + n_z - 2,)),
                dma((writers,)),
                dma((writers,)),
                dma((2,)),
                dma((writers,)),
                dma((writers,)),
            ]
            + held
            + (relay if extra else []),
            compiler_params=pltpu.CompilerParams(
                collective_id=2 + index, has_side_effects=True, vmem_limit_bytes=48 * 2**20
            ),
            name=f"exchange{rows}_{extra}",
        )(*operands)

    branches = [functools.partial(exchange, index) for index in range(len(tiers))]
    squares, heard, done = lax.switch(
        tier[0], branches, outgoing, squares, meta, spill, starts.reshape(1, 128)
    )

    every = velocity.size * n_x * n_y * n_z
    together = math.gcd(writers, 2)
    received = pl.pallas_call(
        functools.partial(finish_kernel, float(every)),
        grid=(writers // together,),
        in_specs=[
            pl.BlockSpec((8, cells_z), lambda s: (0, 0)),
            pl.BlockSpec((together, capacity * comps, width), lambda s: (s, 0, 0)),
        ],
        out_specs=pl.BlockSpec((comps, together, capacity, width), lambda s: (0, s, 0, 0)),
        scratch_shapes=[pltpu.VMEM((8, width), f32)],
        out_shape=jax.ShapeDtypeStruct((comps, writers, capacity, width), f32),
        name="finish",
    )(squares, done)
    return received.reshape(1, 1, comps, writers, capacity, width)


def solution(mesh):
    return jax.shard_map(
        local,
        mesh=mesh,
        in_specs=(
            P(None, "gx", "gy", "wa"),
            P("gx", "gy", "wa", None),
            P("gx", "gy", "wa", None, None),
        ),
        out_specs=P(("gx", "gy"), "wa", None, None, None, None),
        check_vma=False,
    )
```
